32 devices in a mesh: row: 4 (over y, core), col: 8 (over z, x).
Axes of the slice: x: 2, y: 2, z: 4, core: 2. Of those that a mesh axis runs over, the one named last changes fastest.
Arguments:
- eigvecs: float32 [1024, 50176], P('col', 'row'), may hold values from -6 to 6
- span_vectors: float32 [2, 32, 4, 128], P(None, 'row'), may hold values from -6 to 6
- span_offsets: int32 [2, 32], P(None, 'row'), may hold values from 0 to 12543, as said below
- panels: bfloat16 [2, 256, 50176], P(None, 'col', 'row'), may hold values from -0.026785714 to 0.026785714
Outputs:
- back_vectors: float32 [1024, 50176], P('col', 'row')
The draws below stay inside these ranges and needn't reach their ends.
Inputs may be any that keep to these rules, and one draw needn't show every extreme that they name: `span_offsets`: each block starts within the rows of its index of row and ends at most 128 rows after them, and inside the matrix; on every index of row but the last the last block of each sweep reaches into the next index's rows.
All inputs are finite; a program needn't handle non-finite values.
Results may differ from the reference program's by a relative error of at most 0.0075.
Values may be sent and summed in bfloat16 or wider, within the bound.
A program may use at most 128 MiB of HBM per device.

```python
import jax
import jax.numpy as jnp
from jax import lax

K = 1024
ROWS_DEV = 12544
N = 50176
BAND = 128
REFL = 4
SPANS_DEV = 8
SPANS = 32
SWEEPS = 2
WIDTH = 256
PANELS = 2
N_ROW = 4


def draw_span_offsets(key, part):
    key_base, key_last = jax.random.split(key, 2)
    offsets_all = jax.random.randint(key_base, (SWEEPS, N_ROW, SPANS_DEV), 0, ROWS_DEV - BAND + 1)
    last_span = jax.random.randint(key_last, (SWEEPS, N_ROW), ROWS_DEV - 3 * BAND // 4, ROWS_DEV - BAND // 4 + 1)
    device_ids = jnp.arange(N_ROW)[None, :]
    last_span = jnp.where(device_ids < N_ROW - 1, last_span, ROWS_DEV - BAND)
    offsets_all = offsets_all.at[:, :, SPANS_DEV - 1].set(last_span)
    return offsets_all.reshape(SWEEPS, N_ROW * SPANS_DEV).astype(jnp.int32)


def draw_panels(key, part):
    key_own = jax.random.fold_in(key, 17)
    own = jax.random.truncated_normal(key_own, -4.0, 4.0, (PANELS, WIDTH, N), jnp.float32)
    scaled = own * float(N) ** (-0.5)
    limit = 6.0 * float(N) ** (-0.5)
    return jnp.clip(scaled, -limit, limit).astype(jnp.bfloat16)


def levels(own_key, extent, cuts, least, high):
    def one(axis_at, shards_of):
        heights = jax.random.uniform(jax.random.fold_in(jax.random.fold_in(own_key, 6), axis_at), (shards_of,), jnp.float32, least / len(cuts), high / len(cuts))
        return jnp.repeat(jnp.exp(heights), extent[axis_at] // shards_of).reshape((-1,) + (1,) * (len(extent) - axis_at - 1))

    loudness = one(*cuts[0])
    for cut in cuts[1:]:
        loudness = loudness * one(*cut)
    return loudness


def centred(rng, shape, width, reach, cuts=(), held_as=jnp.bfloat16):
    factor_of = levels(rng, shape, cuts, -0.22, 0.18) if cuts else 1.0
    values = jax.random.normal(rng, shape, jnp.float32) * width * factor_of
    return jnp.minimum(jnp.maximum(values, -reach), reach).astype(held_as)


def setup_inputs(seed: int = 0) -> dict:
    streams_of = jax.random.split(jax.random.key(seed), 5)
    return {
        "eigvecs": centred(streams_of[0], (K, N), 1.0, 6.0, ((0, 8), (1, 4)), jnp.float32),
        "span_vectors": centred(streams_of[1], (SWEEPS, SPANS, REFL, BAND), 1.0, 6.0, ((1, 4),), jnp.float32),
        "span_offsets": draw_span_offsets(jax.random.fold_in(streams_of[4], 71), 0),
        "panels": draw_panels(jax.random.fold_in(streams_of[4], 71), 0),
    }


PRECISE = lax.Precision.HIGHEST
CONTRACT_LAST = (((1,), (1,)), ((), ()))
CONTRACT_FIRST = (((0,), (0,)), ((), ()))

def wy_matrix(gram_mat):
    return jnp.triu(gram_mat, 1) + 0.5 * jnp.diag(jnp.diag(gram_mat))

def apply_span(window, vectors):
    gram_mat = jnp.dot(vectors, vectors.T, precision=PRECISE)
    inner = jnp.dot(vectors, window.T, precision=PRECISE)
    coeffs = lax.linalg.triangular_solve(wy_matrix(gram_mat), inner, left_side=True, lower=False)
    return window - jnp.dot(coeffs.T, vectors, precision=PRECISE)

def reference(eigvecs, span_vectors, span_offsets, panels):
    eigen = eigvecs
    for sweep_at in range(SWEEPS):
        vectors = span_vectors[sweep_at]
        offsets = span_offsets[sweep_at]

        def advance(span_at, state, vectors=vectors, offsets=offsets):
            begin_at = (span_at // SPANS_DEV * ROWS_DEV + offsets[span_at]).astype(jnp.int32)
            window = lax.dynamic_slice_in_dim(state, begin_at, BAND, 1)
            return lax.dynamic_update_slice_in_dim(state, apply_span(window, vectors[span_at]), begin_at, 1)
        eigen = lax.fori_loop(0, SPANS, advance, eigen)
    for panel_at in range(PANELS):
        reflect = panels[panel_at]
        gram_mat = lax.dot_general(reflect.astype(jnp.float32), reflect.astype(jnp.float32), CONTRACT_LAST, preferred_element_type=jnp.float32)
        inner = lax.dot_general(reflect.astype(jnp.float32), eigen.astype(jnp.bfloat16).astype(jnp.float32), CONTRACT_LAST, preferred_element_type=jnp.float32)
        coeffs = lax.linalg.triangular_solve(wy_matrix(gram_mat), inner, left_side=True, lower=False)
        eigen = eigen - lax.dot_general(coeffs.astype(jnp.bfloat16).astype(jnp.float32), reflect.astype(jnp.float32), CONTRACT_FIRST, preferred_element_type=jnp.float32)
    return eigen
```

```python
import functools

import jax
import jax.numpy as jnp
from jax import lax
from jax.experimental import pallas as pl
from jax.experimental.pallas import tpu as pltpu
from jax.sharding import PartitionSpec as P

PRECISE = lax.Precision.HIGHEST
LAST = (((1,), (1,)), ((), ()))
INNER = (((1,), (0,)), ((), ()))
LANES = 128
F32 = jnp.float32
BF16 = jnp.bfloat16
UP, DOWN, ACROSS = 0, 1, 2


def tile_of(rows_dev, most):
    count = rows_dev // LANES
    return LANES * max(part for part in range(1, most + 1) if count % part == 0)


def halves(value):
    high = value.astype(BF16)
    return high, (value - high.astype(F32)).astype(BF16)


def dot_split(left, right, dims):
    (left_high, left_low), (right_high, right_low) = left, right
    dot = functools.partial(lax.dot_general, dimension_numbers=dims, preferred_element_type=F32)
    return dot(left_high, right_high) + (dot(left_high, right_low) + dot(left_low, right_high))


def precise_dot(left, right, dims=INNER):
    return lax.dot_general(left, right, dims, precision=PRECISE, preferred_element_type=F32)


def triangle_inverse(matrix, down_at, across_at):
    order = matrix.shape[0]
    same = down_at == across_at
    diagonal = jnp.where(same, matrix, 0.0)
    down = 1.0 / jnp.sum(diagonal, axis=1, keepdims=True)
    across = 1.0 / jnp.sum(diagonal, axis=0, keepdims=True)
    inverse = jnp.where(same, down, 0.0)
    beside = (down_at // 2 == across_at // 2) & (down_at != across_at)
    inverse = inverse - jnp.where(beside, matrix * down * across, 0.0)
    size = 2
    while size < order:
        together = down_at // (2 * size) == across_at // (2 * size)
        beside = together & (down_at // size != across_at // size)
        off = jnp.where(beside, matrix, 0.0)
        inverse = inverse - precise_dot(inverse, precise_dot(off, inverse))
        size *= 2
    return inverse


def kernel(
    eig_ref, vec_ref, off_ref, pan_ref, out_ref,
    eig, wall, low, high, base, tail_out, tail_in, pack, sums, got,
    load_sem, own_sem, recv_sem, send_sem, tail_sem, pack_send, pack_recv, sum_send, sum_recv, out_sem,
):
    rows, cols = lax.axis_size("row"), lax.axis_size("col")
    line = cols // 2
    row, col = lax.axis_index("row"), lax.axis_index("col")
    at, side = col // 2, col % 2
    columns, rows_dev = eig.shape
    panels, _, width_own, _ = wall.shape
    width = cols * width_own
    sweeps, spans, refl, band = vec_ref.shape
    own = sweeps * spans * refl
    total = rows * own
    chunk = tile_of(rows_dev, 14)
    chunks = rows_dev // chunk
    tiles = rows_dev // LANES
    group = tile_of(rows_dev, 7)
    groups = rows_dev // group
    last = panels - 1
    beside = at + 1 - 2 * (at % 2)

    def cut(index):
        return pl.ds(pl.multiple_of(index * chunk, chunk), chunk)

    def target(way):
        if way == ACROSS:
            return {"col": col + 1 - 2 * side}
        return {"col": col + 2 if way == UP else col - 2}

    def copy(way, panel, origin, index, mine=False):
        where = wall.at[panel, origin, :, cut(index)]
        return pltpu.make_async_remote_copy(
            src_ref=pan_ref.at[panel, :, cut(index)] if mine else where,
            dst_ref=where,
            send_sem=send_sem.at[way, panel, origin],
            recv_sem=recv_sem.at[panel, origin, index],
            device_id=target(way),
            device_id_type=pl.DeviceIdType.MESH,
        )

    def send(way, panel, origin, index, mine=False):
        def start():
            copy(way, panel, origin, index, mine).start()

        if way == UP:
            pl.when(at < line - 1)(start)
        elif way == DOWN:
            pl.when(at > 0)(start)
        else:
            start()

    def send_own(way, panel):
        @pl.loop(0, chunks)
        def _(index):
            send(way, panel, col, index, True)

    def arrived(panel, origin, index):
        copy(ACROSS, panel, origin, index).wait_recv()

    def goes_across(panel, origin_at):
        return (origin_at != beside) if panel == last else (origin_at >= 0)

    def serve(panel, step, index):
        for way, source in ((UP, at - step), (DOWN, at + step)):
            @pl.when((source >= 0) & (source < line))
            def _(way=way, source=source):
                origin = 2 * source + side
                arrived(panel, origin, index)
                send(way, panel, origin, index)

                @pl.when(goes_across(panel, source))
                def _():
                    send(ACROSS, panel, origin, index)

    def serve_all(panel, step):
        @pl.loop(0, chunks)
        def _(index):
            serve(panel, step, index)

        if panel < last:
            @pl.when(at == step)
            def _():
                send_own(UP, panel + 1)

            @pl.when(at == line - 1 - step)
            def _():
                send_own(DOWN, panel + 1)

    def serve_partner(index):
        origin = 2 * at + 1 - side
        arrived(last, origin, index)

        @pl.when(at % 2 == 0)
        def _():
            send(UP, last, origin, index)

        @pl.when(at % 2 == 1)
        def _():
            send(DOWN, last, origin, index)

    def from_partner(panel, index):
        for source in range(line):
            def take(source=source):
                arrived(panel, 2 * source + 1 - side, index)

            if panel == last:
                pl.when(at != source)(take)
            else:
                take()

    barrier = pltpu.get_barrier_semaphore()

    def greet(where):
        pl.semaphore_signal(barrier, inc=1, device_id=where, device_id_type=pl.DeviceIdType.MESH)

    greet(target(ACROSS))
    pl.when(at > 0)(lambda: greet(target(DOWN)))
    pl.when(at < line - 1)(lambda: greet(target(UP)))
    for step in range(1, rows):
        greet({"row": lax.rem(row + step, rows)})
    neighbours = jnp.minimum(at, 1) + jnp.minimum(line - 1 - at, 1)
    pl.semaphore_wait(barrier, rows + neighbours)

    send_own(UP, 0)
    send_own(DOWN, 0)
    send_own(ACROSS, 0)
    load = pltpu.make_async_copy(eig_ref, eig, load_sem)
    load.start()
    for panel in range(panels):
        pltpu.make_async_copy(pan_ref.at[panel], wall.at[panel, col], own_sem.at[panel]).start()
    pl.when(at == 0)(lambda: send_own(UP, 1))
    pl.when(at == line - 1)(lambda: send_own(DOWN, 1))

    for index in range(sweeps * spans):
        low[index * refl : (index + 1) * refl, :] = vec_ref[index // spans, index % spans]
    per = 8 // refl
    for index in range(own // 8):
        rows_at = slice(8 * index, 8 * index + 8)
        spread = jnp.concatenate([low[rows_at, :], jnp.zeros((8, LANES), F32)], axis=1)
        moved = jnp.zeros_like(spread)
        first = jnp.zeros((8, LANES), jnp.int32)
        for part in range(per):
            span_at = index * per + part
            begin = off_ref[span_at // spans, span_at % spans]
            tile = begin // LANES
            turned = pltpu.roll(spread, begin - tile * LANES, 1)
            place = lax.broadcasted_iota(jnp.int32, (8, 2 * LANES), 0) // refl
            moved = jnp.where(place == part, turned, moved)
            first = jnp.where(place[:, :LANES] == part, tile, first)
        low[rows_at, :] = moved[:, :LANES]
        high[rows_at, :] = moved[:, LANES:]
        base[rows_at, :] = first

    def spans_at(tile):
        part = jnp.where(base[...] == tile, low[...], 0.0)
        return part + jnp.where(base[...] == tile - 1, high[...], 0.0)

    def spans_group(index):
        first = index * (group // LANES)
        return jnp.concatenate([spans_at(first + step) for step in range(group // LANES)], axis=1)

    def cut_group(index):
        return pl.ds(pl.multiple_of(index * group, group), group)

    tail_out[...] = jnp.where(base[...] == tiles - 1, high[...], 0.0)

    def tail_copy():
        return pltpu.make_async_remote_copy(
            src_ref=tail_out, dst_ref=tail_in, send_sem=tail_sem.at[0], recv_sem=tail_sem.at[1],
            device_id={"row": row + 1}, device_id_type=pl.DeviceIdType.MESH,
        )

    pl.when(row < rows - 1)(lambda: tail_copy().start())
    load.wait()

    def products(index, acc):
        spread = spans_group(index)
        left = jnp.concatenate([eig[:, cut_group(index)], spread], axis=0)
        right = jnp.concatenate([jnp.zeros_like(spread), spread], axis=0)
        return acc + dot_split(halves(left), halves(right), LAST)

    acc = lax.fori_loop(0, groups, products, jnp.zeros((columns + own, 2 * own), F32))
    pl.when(row > 0)(lambda: tail_copy().wait_recv())

    @pl.when(row == 0)
    def _():
        tail_in[...] = jnp.zeros_like(tail_in)

    before = tail_in[...]
    head = spans_at(0)
    nothing = jnp.zeros_like(before)
    left = jnp.concatenate([eig[:, :LANES], head], axis=0)
    acc = acc + dot_split(halves(left), halves(jnp.concatenate([before, nothing], axis=0)), LAST)
    tail = tail_out[...]
    beyond = dot_split(halves(tail), halves(jnp.concatenate([nothing, tail], axis=0)), LAST)
    pack[row, :columns, :] = acc[:columns]
    pack[row, columns : columns + own, :] = acc[columns:] + beyond
    pack[row, columns + own :, :] = dot_split(
        halves(before), halves(jnp.concatenate([head, nothing], axis=0)), LAST
    )

    def pack_copy(step):
        return pltpu.make_async_remote_copy(
            src_ref=pack.at[row], dst_ref=pack.at[row], send_sem=pack_send.at[step], recv_sem=pack_recv.at[row],
            device_id={"row": lax.rem(row + step, rows)}, device_id_type=pl.DeviceIdType.MESH,
        )

    def pack_taken(step):
        source = lax.rem(row + step, rows)
        return pltpu.make_async_remote_copy(
            src_ref=pack.at[source], dst_ref=pack.at[source], send_sem=pack_send.at[step], recv_sem=pack_recv.at[source],
            device_id={"row": source}, device_id_type=pl.DeviceIdType.MESH,
        )

    for step in range(1, rows):
        pack_copy(step).start()
    serve_all(0, 1) if line > 1 else None
    for step in range(1, rows):
        pack_taken(step).wait_recv()

    def placed(value, shift):
        wide = value
        if total > 2 * own:
            zeros = jnp.zeros((value.shape[0], total - 2 * own), F32)
            wide = jnp.concatenate([value, zeros], axis=1)
        shift = shift * own % total
        return pltpu.roll(wide, shift, 1) if shift else wide

    inner = jnp.zeros((columns, total), F32)
    blocks = []
    for index in range(rows):
        inner = inner + placed(pack[index, :columns, :], index - 1)
        block = placed(pack[index, columns : columns + own, :], index - 1)
        if index < rows - 1:
            block = block + placed(pack[index + 1, columns + own :, :], index + 1)
        blocks.append(block)
    matrix = jnp.concatenate(blocks, axis=0)
    orders = []
    for axis in range(2):
        value = lax.broadcasted_iota(jnp.int32, (total, total), axis)
        part, within = value // own, value % own
        sweep_own = spans * refl
        orders.append((within // sweep_own) * (rows * sweep_own) + part * sweep_own + within % sweep_own)
    down, over = orders
    earlier = (down // refl > over // refl) | ((down // refl == over // refl) & (down < over))
    matrix = jnp.where(earlier, matrix, jnp.where(down == over, 0.5 * matrix, 0.0))
    coeffs = precise_dot(inner, triangle_inverse(matrix, down, over), LAST)
    coeffs = pltpu.roll(coeffs, lax.rem(total + own - own * row, total), 1)[:, : 2 * own]
    coeffs = halves(coeffs)
    for step in range(2, line - 1):
        serve_all(0, step)

    @pl.loop(0, groups)
    def _(index):
        spread = spans_group(index)
        right = jnp.concatenate([jnp.zeros_like(spread), spread], axis=0)
        eig[:, cut_group(index)] -= dot_split(coeffs, halves(right), INNER)

    eig[:, :LANES] -= dot_split(coeffs, halves(jnp.concatenate([before, nothing], axis=0)), INNER)
    if line > 2:
        serve_all(0, line - 1)
    for panel in range(1, panels):
        send_own(ACROSS, panel)

    for panel in range(panels):
        pltpu.make_async_copy(pan_ref.at[panel], wall.at[panel, col], own_sem.at[panel]).wait()

    def reflectors(panel, index):
        return jnp.concatenate([wall[panel, part, :, cut(index)] for part in range(cols)], axis=0)

    def add_sums(panel, index):
        reflect = reflectors(panel, index)
        left = jnp.concatenate([eig[:, cut(index)].astype(BF16), reflect], axis=0)
        sums[panel] += lax.dot_general(left, reflect, LAST, preferred_element_type=F32)

    def row_sum(panel):
        step, bit = 0, 1
        while bit < rows:
            low_bit = (row // bit) % 2
            move = pltpu.make_async_remote_copy(
                src_ref=sums.at[panel], dst_ref=got.at[panel, step],
                send_sem=sum_send.at[panel, step], recv_sem=sum_recv.at[panel, step],
                device_id={"row": row + bit * (1 - 2 * low_bit)}, device_id_type=pl.DeviceIdType.MESH,
            )
            move.start()
            move.wait()
            sums[panel] += got[panel, step]
            step, bit = step + 1, 2 * bit

    def solved(panel):
        down = lax.broadcasted_iota(jnp.int32, (width, width), 0)
        over = lax.broadcasted_iota(jnp.int32, (width, width), 1)
        gram = sums[panel, columns:, :]
        matrix = jnp.where(down < over, gram, jnp.where(down == over, 0.5 * gram, 0.0))
        inverse = triangle_inverse(matrix, down, over)
        return precise_dot(sums[panel, :columns, :], inverse, LAST).astype(BF16)

    def update(panel, index, coeffs):
        eig[:, cut(index)] -= lax.dot_general(coeffs, reflectors(panel, index), INNER, preferred_element_type=F32)

    for panel in range(panels):
        sums[panel] = jnp.zeros_like(sums[panel])

    @pl.loop(0, chunks)
    def _(index):
        from_partner(0, index)
        add_sums(0, index)
        if line > 1:
            serve(1, 1, index)

    row_sum(0)
    coeffs = solved(0)

    @pl.loop(0, chunks)
    def _(index):
        serve_partner(index)
        for step in range(2, line - 1):
            serve(1, step, index)
        update(0, index, coeffs)

    if line > 2:
        @pl.loop(0, chunks)
        def _(index):
            serve(1, line - 1, index)

    @pl.loop(0, chunks)
    def _(index):
        from_partner(1, index)
        add_sums(1, index)

    row_sum(1)
    coeffs = solved(1)

    def out_copy(index):
        return pltpu.make_async_copy(eig.at[:, cut(index)], out_ref.at[:, cut(index)], out_sem.at[index])

    @pl.loop(0, chunks)
    def _(index):
        update(1, index, coeffs)
        out_copy(index).start()

    def gone(way, panel, origin):
        def wait():
            piece = wall.at[panel, origin]
            pltpu.make_async_remote_copy(
                src_ref=piece, dst_ref=piece, send_sem=send_sem.at[way, panel, origin],
                recv_sem=recv_sem.at[panel, origin, 0], device_id=target(way),
                device_id_type=pl.DeviceIdType.MESH,
            ).wait_send()

        if way == UP:
            pl.when(at < line - 1)(wait)
        elif way == DOWN:
            pl.when(at > 0)(wait)
        else:
            wait()

    for panel in range(panels):
        for source in range(line):
            origin = 2 * source + side
            pl.when(at >= source)(lambda: gone(UP, panel, origin))
            pl.when(at <= source)(lambda: gone(DOWN, panel, origin))
            pl.when(goes_across(panel, jnp.int32(source)))(lambda: gone(ACROSS, panel, origin))
    pl.when(at % 2 == 0)(lambda: gone(UP, last, 2 * at + 1 - side))
    pl.when(at % 2 == 1)(lambda: gone(DOWN, last, 2 * at + 1 - side))
    pl.when(row < rows - 1)(lambda: tail_copy().wait_send())
    for step in range(1, rows):
        pack_copy(step).wait_send()

    @pl.loop(0, chunks)
    def _(index):
        out_copy(index).wait()


def local(eigvecs, span_vectors, span_offsets, panels):
    rows, cols = lax.axis_size("row"), lax.axis_size("col")
    columns, rows_dev = eigvecs.shape
    count, width_own, _ = panels.shape
    sweeps, spans, refl, band = span_vectors.shape
    own = sweeps * spans * refl
    width = width_own * cols
    steps = rows.bit_length() - 1
    chunks = rows_dev // tile_of(rows_dev, 14)
    vmem = pltpu.VMEM
    dma = pltpu.SemaphoreType.DMA
    return pl.pallas_call(
        kernel,
        out_shape=jax.ShapeDtypeStruct(eigvecs.shape, F32),
        in_specs=[
            pl.BlockSpec(memory_space=pl.ANY),
            pl.BlockSpec(memory_space=pltpu.VMEM),
            pl.BlockSpec(memory_space=pltpu.SMEM),
            pl.BlockSpec(memory_space=pl.ANY),
        ],
        out_specs=pl.BlockSpec(memory_space=pl.ANY),
        scratch_shapes=[
            vmem((columns, rows_dev), F32),
            vmem((count, cols, width_own, rows_dev), BF16),
            vmem((own, LANES), F32),
            vmem((own, LANES), F32),
            vmem((own, LANES), jnp.int32),
            vmem((own, LANES), F32),
            vmem((own, LANES), F32),
            vmem((rows, columns + 2 * own, 2 * own), F32),
            vmem((count, columns + width, width), F32),
            vmem((count, steps, columns + width, width), F32),
            dma,
            dma((count,)),
            dma((count, cols, chunks)),
            dma((3, count, cols)),
            dma((2,)),
            dma((rows,)),
            dma((rows,)),
            dma((count, steps)),
            dma((count, steps)),
            dma((chunks,)),
        ],
        compiler_params=pltpu.CompilerParams(
            collective_id=0, has_side_effects=True, vmem_limit_bytes=60 * 2**20
        ),
        cost_estimate=pl.CostEstimate(
            flops=8 * width * (width + columns) * rows_dev,
            bytes_accessed=8 * rows_dev * columns + 8 * width * rows_dev,
            transcendentals=0,
        ),
    )(eigvecs, span_vectors, span_offsets, panels)


def solution(mesh):
    return jax.shard_map(
        local,
        mesh=mesh,
        in_specs=(
            P("col", "row"),
            P(None, "row", None, None),
            P(None, "row"),
            P(None, "col", "row"),
        ),
        out_specs=P("col", "row"),
        check_vma=False,
    )
```

```python
import functools

import jax
import jax.numpy as jnp
from jax import lax
from jax.experimental import pallas as pl
from jax.experimental.pallas import tpu as pltpu
from jax.sharding import PartitionSpec as P

PRECISE = lax.Precision.HIGHEST
LAST = (((1,), (1,)), ((), ()))
INNER = (((1,), (0,)), ((), ()))
LANES = 128
F32 = jnp.float32
BF16 = jnp.bfloat16
UP, DOWN, ACROSS = 0, 1, 2


def tile_of(rows_dev, most):
    count = rows_dev // LANES
    return LANES * max(part for part in range(1, most + 1) if count % part == 0)


def halves(value):
    high = value.astype(BF16)
    return high, (value - high.astype(F32)).astype(BF16)


def dot_split(left, right, dims):
    (left_high, left_low), (right_high, right_low) = left, right
    dot = functools.partial(lax.dot_general, dimension_numbers=dims, preferred_element_type=F32)
    return dot(left_high, right_high) + (dot(left_high, right_low) + dot(left_low, right_high))


def precise_dot(left, right, dims=INNER):
    return lax.dot_general(left, right, dims, precision=PRECISE, preferred_element_type=F32)


def triangle_inverse(matrix, down_at, across_at):
    order = matrix.shape[0]
    same = down_at == across_at
    diagonal = jnp.where(same, matrix, 0.0)
    down = 1.0 / jnp.sum(diagonal, axis=1, keepdims=True)
    across = 1.0 / jnp.sum(diagonal, axis=0, keepdims=True)
    inverse = jnp.where(same, down, 0.0)
    beside = (down_at // 2 == across_at // 2) & (down_at != across_at)
    inverse = inverse - jnp.where(beside, matrix * down * across, 0.0)
    size = 2
    while size < order:
        together = down_at // (2 * size) == across_at // (2 * size)
        beside = together & (down_at // size != across_at // size)
        off = jnp.where(beside, matrix, 0.0)
        inverse = inverse - precise_dot(inverse, precise_dot(off, inverse))
        size *= 2
    return inverse


def kernel(
    eig_ref, vec_ref, off_ref, pan_ref, eig, wall_last, coef_ref,
    wall_first, low, high, base, tail_out, tail_in, pack, sums, got,
    load_sem, own_sem, recv_sem, send_sem, tail_sem, pack_send, pack_recv, sum_send, sum_recv,
):
    rows, cols = lax.axis_size("row"), lax.axis_size("col")
    line = cols // 2
    row, col = lax.axis_index("row"), lax.axis_index("col")
    at, side = col // 2, col % 2
    columns, rows_dev = eig.shape
    walls = (wall_first, wall_last)
    panels, width_own, _ = pan_ref.shape
    width = cols * width_own
    sweeps, spans, refl, band = vec_ref.shape
    own = sweeps * spans * refl
    total = rows * own
    chunk = tile_of(rows_dev, 14)
    chunks = rows_dev // chunk
    tiles = rows_dev // LANES
    group = tile_of(rows_dev, 7)
    groups = rows_dev // group
    last = panels - 1
    beside = at + 1 - 2 * (at % 2)

    def cut(index):
        return pl.ds(pl.multiple_of(index * chunk, chunk), chunk)

    def target(way):
        if way == ACROSS:
            return {"col": col + 1 - 2 * side}
        return {"col": col + 2 if way == UP else col - 2}

    def copy(way, panel, origin, index, mine=False):
        where = walls[panel].at[origin, :, cut(index)]
        return pltpu.make_async_remote_copy(
            src_ref=pan_ref.at[panel, :, cut(index)] if mine else where,
            dst_ref=where,
            send_sem=send_sem.at[way, panel, origin],
            recv_sem=recv_sem.at[panel, origin, index],
            device_id=target(way),
            device_id_type=pl.DeviceIdType.MESH,
        )

    def send(way, panel, origin, index, mine=False):
        def start():
            copy(way, panel, origin, index, mine).start()

        if way == UP:
            pl.when(at < line - 1)(start)
        elif way == DOWN:
            pl.when(at > 0)(start)
        else:
            start()

    def send_own(way, panel):
        @pl.loop(0, chunks)
        def _(index):
            send(way, panel, col, index, True)

    def arrived(panel, origin, index):
        copy(ACROSS, panel, origin, index).wait_recv()

    def goes_across(panel, origin_at):
        return (origin_at != beside) if panel == last else (origin_at >= 0)

    def serve(panel, step, index):
        for way, source in ((UP, at - step), (DOWN, at + step)):
            @pl.when((source >= 0) & (source < line))
            def _(way=way, source=source):
                origin = 2 * source + side
                arrived(panel, origin, index)
                send(way, panel, origin, index)

                @pl.when(goes_across(panel, source))
                def _():
                    send(ACROSS, panel, origin, index)

    def serve_all(panel, step):
        @pl.loop(0, chunks)
        def _(index):
            serve(panel, step, index)

        if panel < last:
            @pl.when(at == step)
            def _():
                send_own(UP, panel + 1)

            @pl.when(at == line - 1 - step)
            def _():
                send_own(DOWN, panel + 1)

    def serve_partner(index):
        origin = 2 * at + 1 - side
        arrived(last, origin, index)

        @pl.when(at % 2 == 0)
        def _():
            send(UP, last, origin, index)

        @pl.when(at % 2 == 1)
        def _():
            send(DOWN, last, origin, index)

    def from_partner(panel, index):
        for source in range(line):
            def take(source=source):
                arrived(panel, 2 * source + 1 - side, index)

            if panel == last:
                pl.when(at != source)(take)
            else:
                take()

    barrier = pltpu.get_barrier_semaphore()

    def greet(where):
        pl.semaphore_signal(barrier, inc=1, device_id=where, device_id_type=pl.DeviceIdType.MESH)

    greet(target(ACROSS))
    pl.when(at > 0)(lambda: greet(target(DOWN)))
    pl.when(at < line - 1)(lambda: greet(target(UP)))
    for step in range(1, rows):
        greet({"row": lax.rem(row + step, rows)})
    neighbours = jnp.minimum(at, 1) + jnp.minimum(line - 1 - at, 1)
    pl.semaphore_wait(barrier, rows + neighbours)

    send_own(UP, 0)
    send_own(DOWN, 0)
    send_own(ACROSS, 0)
    load = pltpu.make_async_copy(eig_ref, eig, load_sem)
    load.start()
    for panel in range(panels):
        pltpu.make_async_copy(pan_ref.at[panel], walls[panel].at[col], own_sem.at[panel]).start()
    pl.when(at == 0)(lambda: send_own(UP, 1))
    pl.when(at == line - 1)(lambda: send_own(DOWN, 1))

    for index in range(sweeps * spans):
        low[index * refl : (index + 1) * refl, :] = vec_ref[index // spans, index % spans]
    per = 8 // refl
    for index in range(own // 8):
        rows_at = slice(8 * index, 8 * index + 8)
        spread = jnp.concatenate([low[rows_at, :], jnp.zeros((8, LANES), F32)], axis=1)
        moved = jnp.zeros_like(spread)
        first = jnp.zeros((8, LANES), jnp.int32)
        for part in range(per):
            span_at = index * per + part
            begin = off_ref[span_at // spans, span_at % spans]
            tile = begin // LANES
            turned = pltpu.roll(spread, begin - tile * LANES, 1)
            place = lax.broadcasted_iota(jnp.int32, (8, 2 * LANES), 0) // refl
            moved = jnp.where(place == part, turned, moved)
            first = jnp.where(place[:, :LANES] == part, tile, first)
        low[rows_at, :] = moved[:, :LANES]
        high[rows_at, :] = moved[:, LANES:]
        base[rows_at, :] = first

    def spans_at(tile):
        part = jnp.where(base[...] == tile, low[...], 0.0)
        return part + jnp.where(base[...] == tile - 1, high[...], 0.0)

    def spans_group(index):
        first = index * (group // LANES)
        return jnp.concatenate([spans_at(first + step) for step in range(group // LANES)], axis=1)

    def cut_group(index):
        return pl.ds(pl.multiple_of(index * group, group), group)

    tail_out[...] = jnp.where(base[...] == tiles - 1, high[...], 0.0)

    def tail_copy():
        return pltpu.make_async_remote_copy(
            src_ref=tail_out, dst_ref=tail_in, send_sem=tail_sem.at[0], recv_sem=tail_sem.at[1],
            device_id={"row": row + 1}, device_id_type=pl.DeviceIdType.MESH,
        )

    pl.when(row < rows - 1)(lambda: tail_copy().start())
    load.wait()

    def products(index, acc):
        spread = spans_group(index)
        left = jnp.concatenate([eig[:, cut_group(index)], spread], axis=0)
        right = jnp.concatenate([jnp.zeros_like(spread), spread], axis=0)
        return acc + dot_split(halves(left), halves(right), LAST)

    acc = lax.fori_loop(0, groups, products, jnp.zeros((columns + own, 2 * own), F32))
    pl.when(row > 0)(lambda: tail_copy().wait_recv())

    @pl.when(row == 0)
    def _():
        tail_in[...] = jnp.zeros_like(tail_in)

    before = tail_in[...]
    head = spans_at(0)
    nothing = jnp.zeros_like(before)
    left = jnp.concatenate([eig[:, :LANES], head], axis=0)
    acc = acc + dot_split(halves(left), halves(jnp.concatenate([before, nothing], axis=0)), LAST)
    tail = tail_out[...]
    beyond = dot_split(halves(tail), halves(jnp.concatenate([nothing, tail], axis=0)), LAST)
    pack[row, :columns, :] = acc[:columns]
    pack[row, columns : columns + own, :] = acc[columns:] + beyond
    pack[row, columns + own :, :] = dot_split(
        halves(before), halves(jnp.concatenate([head, nothing], axis=0)), LAST
    )

    def pack_copy(step):
        return pltpu.make_async_remote_copy(
            src_ref=pack.at[row], dst_ref=pack.at[row], send_sem=pack_send.at[step], recv_sem=pack_recv.at[row],
            device_id={"row": lax.rem(row + step, rows)}, device_id_type=pl.DeviceIdType.MESH,
        )

    def pack_taken(step):
        source = lax.rem(row + step, rows)
        return pltpu.make_async_remote_copy(
            src_ref=pack.at[source], dst_ref=pack.at[source], send_sem=pack_send.at[step], recv_sem=pack_recv.at[source],
            device_id={"row": source}, device_id_type=pl.DeviceIdType.MESH,
        )

    for step in range(1, rows):
        pack_copy(step).start()
    serve_all(0, 1) if line > 1 else None
    for step in range(1, rows):
        pack_taken(step).wait_recv()

    def placed(value, shift):
        wide = value
        if total > 2 * own:
            zeros = jnp.zeros((value.shape[0], total - 2 * own), F32)
            wide = jnp.concatenate([value, zeros], axis=1)
        shift = shift * own % total
        return pltpu.roll(wide, shift, 1) if shift else wide

    inner = jnp.zeros((columns, total), F32)
    blocks = []
    for index in range(rows):
        inner = inner + placed(pack[index, :columns, :], index - 1)
        block = placed(pack[index, columns : columns + own, :], index - 1)
        if index < rows - 1:
            block = block + placed(pack[index + 1, columns + own :, :], index + 1)
        blocks.append(block)
    matrix = jnp.concatenate(blocks, axis=0)
    orders = []
    for axis in range(2):
        value = lax.broadcasted_iota(jnp.int32, (total, total), axis)
        part, within = value // own, value % own
        sweep_own = spans * refl
        orders.append((within // sweep_own) * (rows * sweep_own) + part * sweep_own + within % sweep_own)
    down, over = orders
    earlier = (down // refl > over // refl) | ((down // refl == over // refl) & (down < over))
    matrix = jnp.where(earlier, matrix, jnp.where(down == over, 0.5 * matrix, 0.0))
    coeffs = precise_dot(inner, triangle_inverse(matrix, down, over), LAST)
    coeffs = pltpu.roll(coeffs, lax.rem(total + own - own * row, total), 1)[:, : 2 * own]
    coeffs = halves(coeffs)
    for step in range(2, line - 1):
        serve_all(0, step)

    @pl.loop(0, groups)
    def _(index):
        spread = spans_group(index)
        right = jnp.concatenate([jnp.zeros_like(spread), spread], axis=0)
        eig[:, cut_group(index)] -= dot_split(coeffs, halves(right), INNER)

    eig[:, :LANES] -= dot_split(coeffs, halves(jnp.concatenate([before, nothing], axis=0)), INNER)
    if line > 2:
        serve_all(0, line - 1)
    for panel in range(1, panels):
        send_own(ACROSS, panel)

    for panel in range(panels):
        pltpu.make_async_copy(pan_ref.at[panel], walls[panel].at[col], own_sem.at[panel]).wait()

    def reflectors(panel, index):
        return jnp.concatenate([walls[panel][part, :, cut(index)] for part in range(cols)], axis=0)

    def add_sums(panel, index):
        reflect = reflectors(panel, index)
        left = jnp.concatenate([eig[:, cut(index)].astype(BF16), reflect], axis=0)
        sums[panel] += lax.dot_general(left, reflect, LAST, preferred_element_type=F32)

    def row_move(panel, step):
        bit = 2**step
        low_bit = (row // bit) % 2
        return pltpu.make_async_remote_copy(
            src_ref=sums.at[panel], dst_ref=got.at[panel, step],
            send_sem=sum_send.at[panel, step], recv_sem=sum_recv.at[panel, step],
            device_id={"row": row + bit * (1 - 2 * low_bit)}, device_id_type=pl.DeviceIdType.MESH,
        )

    steps = rows.bit_length() - 1

    def row_sum(panel, meanwhile=lambda: None):
        for step in range(steps):
            row_move(panel, step).start()
            if step == steps - 1:
                meanwhile()
            row_move(panel, step).wait()
            sums[panel] += got[panel, step]

    def solved(panel):
        down = lax.broadcasted_iota(jnp.int32, (width, width), 0)
        over = lax.broadcasted_iota(jnp.int32, (width, width), 1)
        gram = sums[panel, columns:, :]
        matrix = jnp.where(down < over, gram, jnp.where(down == over, 0.5 * gram, 0.0))
        inverse = triangle_inverse(matrix, down, over)
        return precise_dot(sums[panel, :columns, :], inverse, LAST).astype(BF16)

    def update(panel, index, coeffs):
        eig[:, cut(index)] -= lax.dot_general(coeffs, reflectors(panel, index), INNER, preferred_element_type=F32)

    for panel in range(panels):
        sums[panel] = jnp.zeros_like(sums[panel])

    @pl.loop(0, chunks)
    def _(index):
        from_partner(0, index)
        add_sums(0, index)
        if line > 1:
            serve(1, 1, index)

    def serve_between():
        for step in range(2, line - 1):
            @pl.loop(0, chunks)
            def _(index):
                serve(1, step, index)

        @pl.loop(0, chunks)
        def _(index):
            serve_partner(index)

    row_sum(0, serve_between)
    coeffs = solved(0)

    @pl.loop(0, chunks)
    def _(index):
        update(0, index, coeffs)

    if line > 2:
        @pl.loop(0, chunks)
        def _(index):
            serve(1, line - 1, index)

    @pl.loop(0, chunks)
    def _(index):
        from_partner(1, index)
        add_sums(1, index)

    row_sum(1)
    coef_ref[...] = solved(1)

    def gone(way, panel, origin):
        def wait():
            piece = walls[panel].at[origin]
            pltpu.make_async_remote_copy(
                src_ref=piece, dst_ref=piece, send_sem=send_sem.at[way, panel, origin],
                recv_sem=recv_sem.at[panel, origin, 0], device_id=target(way),
                device_id_type=pl.DeviceIdType.MESH,
            ).wait_send()

        if way == UP:
            pl.when(at < line - 1)(wait)
        elif way == DOWN:
            pl.when(at > 0)(wait)
        else:
            wait()

    for panel in range(panels):
        for source in range(line):
            origin = 2 * source + side
            pl.when(at >= source)(lambda: gone(UP, panel, origin))
            pl.when(at <= source)(lambda: gone(DOWN, panel, origin))
            pl.when(goes_across(panel, jnp.int32(source)))(lambda: gone(ACROSS, panel, origin))
    pl.when(at % 2 == 0)(lambda: gone(UP, last, 2 * at + 1 - side))
    pl.when(at % 2 == 1)(lambda: gone(DOWN, last, 2 * at + 1 - side))
    pl.when(row < rows - 1)(lambda: tail_copy().wait_send())
    for step in range(1, rows):
        pack_copy(step).wait_send()


def finish_kernel(eig_ref, wall_ref, coef_ref, out_ref, held, sems):
    cols = wall_ref.shape[0]
    rows_dev = eig_ref.shape[1]
    chunk = tile_of(rows_dev, 14)
    chunks = rows_dev // chunk

    def cut(index):
        return pl.ds(pl.multiple_of(index * chunk, chunk), chunk)

    def copy(index):
        return pltpu.make_async_copy(held.at[:, cut(index)], out_ref.at[:, cut(index)], sems.at[index])

    coeffs = coef_ref[...]

    @pl.loop(0, chunks)
    def _(index):
        reflect = jnp.concatenate([wall_ref[part, :, cut(index)] for part in range(cols)], axis=0)
        update = lax.dot_general(coeffs, reflect, INNER, preferred_element_type=F32)
        held[:, cut(index)] = eig_ref[:, cut(index)] - update
        copy(index).start()

    @pl.loop(0, chunks)
    def _(index):
        copy(index).wait()


def local(eigvecs, span_vectors, span_offsets, panels):
    rows, cols = lax.axis_size("row"), lax.axis_size("col")
    columns, rows_dev = eigvecs.shape
    count, width_own, _ = panels.shape
    sweeps, spans, refl, band = span_vectors.shape
    own = sweeps * spans * refl
    width = width_own * cols
    steps = rows.bit_length() - 1
    chunks = rows_dev // tile_of(rows_dev, 14)
    vmem = pltpu.VMEM
    dma = pltpu.SemaphoreType.DMA
    eigen, wall, coeffs = pl.pallas_call(
        kernel,
        out_shape=(
            vmem(eigvecs.shape, F32),
            vmem((cols, width_own, rows_dev), BF16),
            vmem((columns, width), BF16),
        ),
        in_specs=[
            pl.BlockSpec(memory_space=pltpu.HBM),
            pl.BlockSpec(memory_space=pltpu.VMEM),
            pl.BlockSpec(memory_space=pltpu.SMEM),
            pl.BlockSpec(memory_space=pltpu.HBM),
        ],
        out_specs=[pl.BlockSpec(memory_space=pltpu.VMEM)] * 3,
        scratch_shapes=[
            vmem((cols, width_own, rows_dev), BF16),
            vmem((own, LANES), F32),
            vmem((own, LANES), F32),
            vmem((own, LANES), jnp.int32),
            vmem((own, LANES), F32),
            vmem((own, LANES), F32),
            vmem((rows, columns + 2 * own, 2 * own), F32),
            vmem((count, columns + width, width), F32),
            vmem((count, steps, columns + width, width), F32),
            dma,
            dma((count,)),
            dma((count, cols, chunks)),
            dma((3, count, cols)),
            dma((2,)),
            dma((rows,)),
            dma((rows,)),
            dma((count, steps)),
            dma((count, steps)),
        ],
        compiler_params=pltpu.CompilerParams(
            collective_id=0, has_side_effects=True, vmem_limit_bytes=40 * 2**20
        ),
        cost_estimate=pl.CostEstimate(
            flops=8 * width * (width + columns) * rows_dev,
            bytes_accessed=8 * rows_dev * columns + 8 * width * rows_dev,
            transcendentals=0,
        ),
    )(eigvecs, span_vectors, span_offsets, panels)
    return pl.pallas_call(
        finish_kernel,
        out_shape=jax.ShapeDtypeStruct(eigvecs.shape, F32),
        in_specs=[pl.BlockSpec(memory_space=pltpu.VMEM)] * 3,
        out_specs=pl.BlockSpec(memory_space=pl.ANY),
        scratch_shapes=[vmem(eigvecs.shape, F32), dma((chunks,))],
        compiler_params=pltpu.CompilerParams(vmem_limit_bytes=16 * 2**20),
        cost_estimate=pl.CostEstimate(
            flops=2 * width * columns * rows_dev, bytes_accessed=8 * columns * rows_dev, transcendentals=0
        ),
    )(eigen, wall, coeffs)


def solution(mesh):
    return jax.shard_map(
        local,
        mesh=mesh,
        in_specs=(
            P("col", "row"),
            P(None, "row", None, None),
            P(None, "row"),
            P(None, "col", "row"),
        ),
        out_specs=P("col", "row"),
        check_vma=False,
    )
```

```python
import functools

import jax
import jax.numpy as jnp
from jax import lax
from jax.experimental import pallas as pl
from jax.experimental.pallas import tpu as pltpu
from jax.sharding import PartitionSpec as P

PRECISE = lax.Precision.HIGHEST
LAST = (((1,), (1,)), ((), ()))
INNER = (((1,), (0,)), ((), ()))
LANES = 128
F32 = jnp.float32
BF16 = jnp.bfloat16
UP, DOWN, ACROSS = 0, 1, 2


def tile_of(rows_dev, most):
    count = rows_dev // LANES
    return LANES * max(part for part in range(1, most + 1) if count % part == 0)


def halves(value):
    high = value.astype(BF16)
    return high, (value - high.astype(F32)).astype(BF16)


def dot_split(left, right, dims):
    (left_high, left_low), (right_high, right_low) = left, right
    dot = functools.partial(lax.dot_general, dimension_numbers=dims, preferred_element_type=F32)
    return dot(left_high, right_high) + (dot(left_high, right_low) + dot(left_low, right_high))


def precise_dot(left, right, dims=INNER):
    return lax.dot_general(left, right, dims, precision=PRECISE, preferred_element_type=F32)


def triangle_inverse(matrix, down_at, across_at, order):
    same = down_at == across_at
    diagonal = jnp.where(same, matrix, 0.0)
    down = 1.0 / jnp.sum(diagonal, axis=1, keepdims=True)
    across = 1.0 / jnp.sum(diagonal, axis=0, keepdims=True)
    inverse = jnp.where(same, down, 0.0)
    beside = (down_at // 2 == across_at // 2) & (down_at != across_at)
    inverse = inverse - jnp.where(beside, matrix * down * across, 0.0)
    size = 2
    while size < order:
        together = down_at // (2 * size) == across_at // (2 * size)
        beside = together & (down_at // size != across_at // size)
        off = jnp.where(beside, matrix, 0.0)
        inverse = inverse - precise_dot(inverse, precise_dot(off, inverse))
        size *= 2
    return inverse


def last_order(cols, col):
    line, at, side = cols // 2, col // 2, col % 2
    beside = at + 1 - 2 * (at % 2)
    far = (line - 1) * (1 - 2 * at // line)
    first, second = jnp.minimum(beside, far), jnp.maximum(beside, far)
    early = []
    for index in range(line - 2):
        place = index + jnp.where(first <= index, 1, 0)
        early.append(place + jnp.where(second <= place, 1, 0))
    order = [2 * place + side for place in range(line)]
    return order + [2 * place + 1 - side for place in (*early, beside, far)]


def kernel(
    eig_ref, vec_ref, off_ref, pan_ref, eig, wall_last, coef_ref,
    wall_first, vecs, offs, low, high, base, tail_out, tail_in, pack, sums, got, late, late_got, corner, places,
    load_sem, own_sem, recv_sem, send_sem, tail_sem, pack_send, pack_recv, sum_send, sum_recv,
    late_send, late_recv, corner_send, corner_recv,
):
    rows, cols = lax.axis_size("row"), lax.axis_size("col")
    line = cols // 2
    row, col = lax.axis_index("row"), lax.axis_index("col")
    at, side = col // 2, col % 2
    columns, rows_dev = eig.shape
    walls = (wall_first, wall_last)
    panels, width_own, _ = pan_ref.shape
    width = cols * width_own
    sweeps, spans, refl, band = vecs.shape
    own = sweeps * spans * refl
    total = rows * own
    chunk = tile_of(rows_dev, 14)
    chunks = rows_dev // chunk
    tiles = rows_dev // LANES
    group = tile_of(rows_dev, 7)
    groups = rows_dev // group
    last = panels - 1
    beside = at + 1 - 2 * (at % 2)
    order = last_order(cols, col)
    late_width = 2 * width_own
    early_width = width - late_width
    fold = width_own // 8

    def cut(index):
        return pl.ds(pl.multiple_of(index * chunk, chunk), chunk)

    def target(way):
        if way == ACROSS:
            return {"col": col + 1 - 2 * side}
        return {"col": col + 2 if way == UP else col - 2}

    def copy(way, panel, origin, index, mine=False):
        where = walls[panel].at[origin, :, cut(index)]
        return pltpu.make_async_remote_copy(
            src_ref=pan_ref.at[panel, :, cut(index)] if mine else where,
            dst_ref=where,
            send_sem=send_sem.at[way, panel, origin],
            recv_sem=recv_sem.at[panel, origin, index],
            device_id=target(way),
            device_id_type=pl.DeviceIdType.MESH,
        )

    def send(way, panel, origin, index, mine=False):
        def start():
            copy(way, panel, origin, index, mine).start()

        if way == UP:
            pl.when(at < line - 1)(start)
        elif way == DOWN:
            pl.when(at > 0)(start)
        else:
            start()

    def send_own(way, panel):
        @pl.loop(0, chunks)
        def _(index):
            send(way, panel, col, index, True)

    def arrived(panel, origin, index):
        copy(ACROSS, panel, origin, index).wait_recv()

    def goes_across(panel, origin_at):
        return (origin_at != beside) if panel == last else (origin_at >= 0)

    def serve(panel, step, index):
        for way, source in ((UP, at - step), (DOWN, at + step)):
            @pl.when((source >= 0) & (source < line))
            def _(way=way, source=source):
                origin = 2 * source + side
                arrived(panel, origin, index)
                send(way, panel, origin, index)

                @pl.when(goes_across(panel, source))
                def _():
                    send(ACROSS, panel, origin, index)

    def serve_all(panel, step):
        @pl.loop(0, chunks)
        def _(index):
            serve(panel, step, index)

        if panel < last:
            @pl.when(at == step)
            def _():
                send_own(UP, panel + 1)

            @pl.when(at == line - 1 - step)
            def _():
                send_own(DOWN, panel + 1)

    def serve_partner(index):
        origin = 2 * at + 1 - side
        arrived(last, origin, index)

        @pl.when(at % 2 == 0)
        def _():
            send(UP, last, origin, index)

        @pl.when(at % 2 == 1)
        def _():
            send(DOWN, last, origin, index)

    vec_load = pltpu.make_async_copy(vec_ref, vecs, load_sem.at[1])
    off_load = pltpu.make_async_copy(off_ref, offs, load_sem.at[2])
    vec_load.start()
    off_load.start()

    barrier = pltpu.get_barrier_semaphore()

    def greet(where):
        pl.semaphore_signal(barrier, inc=1, device_id=where, device_id_type=pl.DeviceIdType.MESH)

    greet(target(ACROSS))
    pl.when(at > 0)(lambda: greet(target(DOWN)))
    pl.when(at < line - 1)(lambda: greet(target(UP)))
    for step in range(1, rows):
        greet({"row": lax.rem(row + step, rows)})
    neighbours = jnp.minimum(at, 1) + jnp.minimum(line - 1 - at, 1)
    pl.semaphore_wait(barrier, rows + neighbours)

    send_own(UP, 0)
    send_own(DOWN, 0)
    send_own(ACROSS, 0)
    load = pltpu.make_async_copy(eig_ref, eig, load_sem.at[0])
    load.start()
    for panel in range(panels):
        pltpu.make_async_copy(pan_ref.at[panel], walls[panel].at[col], own_sem.at[panel]).start()
    pl.when(at == 0)(lambda: send_own(UP, 1))
    pl.when(at == line - 1)(lambda: send_own(DOWN, 1))

    vec_load.wait()
    off_load.wait()

    for index in range(sweeps * spans):
        low[index * refl : (index + 1) * refl, :] = vecs[index // spans, index % spans]
    per = 8 // refl
    for index in range(own // 8):
        rows_at = slice(8 * index, 8 * index + 8)
        spread = jnp.concatenate([low[rows_at, :], jnp.zeros((8, LANES), F32)], axis=1)
        moved = jnp.zeros_like(spread)
        first = jnp.zeros((8, LANES), jnp.int32)
        for part in range(per):
            span_at = index * per + part
            begin = offs[span_at // spans, span_at % spans]
            tile = begin // LANES
            turned = pltpu.roll(spread, begin - tile * LANES, 1)
            place = lax.broadcasted_iota(jnp.int32, (8, 2 * LANES), 0) // refl
            moved = jnp.where(place == part, turned, moved)
            first = jnp.where(place[:, :LANES] == part, tile, first)
        low[rows_at, :] = moved[:, :LANES]
        high[rows_at, :] = moved[:, LANES:]
        base[rows_at, :] = first

    def spans_at(tile):
        part = jnp.where(base[...] == tile, low[...], 0.0)
        return part + jnp.where(base[...] == tile - 1, high[...], 0.0)

    def spans_group(index):
        first = index * (group // LANES)
        return jnp.concatenate([spans_at(first + step) for step in range(group // LANES)], axis=1)

    def cut_group(index):
        return pl.ds(pl.multiple_of(index * group, group), group)

    tail_out[...] = jnp.where(base[...] == tiles - 1, high[...], 0.0)

    def tail_copy():
        return pltpu.make_async_remote_copy(
            src_ref=tail_out, dst_ref=tail_in, send_sem=tail_sem.at[0], recv_sem=tail_sem.at[1],
            device_id={"row": row + 1}, device_id_type=pl.DeviceIdType.MESH,
        )

    pl.when(row < rows - 1)(lambda: tail_copy().start())
    for panel in range(panels):
        pltpu.make_async_copy(pan_ref.at[panel], walls[panel].at[col], own_sem.at[panel]).wait()

    def own_products(index, acc):
        mine = walls[last][col, :, cut(index)]
        padded = jnp.concatenate([mine, jnp.zeros((LANES - width_own, chunk), BF16)], axis=0)
        return acc + lax.dot_general(mine, padded, LAST, preferred_element_type=F32)

    pack[row, columns + 2 * own :, :] = lax.fori_loop(0, chunks, own_products, jnp.zeros((width_own, LANES), F32))
    load.wait()

    def products(index, acc):
        spread = spans_group(index)
        left = jnp.concatenate([eig[:, cut_group(index)], spread], axis=0)
        right = jnp.concatenate([jnp.zeros_like(spread), spread], axis=0)
        return acc + dot_split(halves(left), halves(right), LAST)

    acc = lax.fori_loop(0, groups, products, jnp.zeros((columns + own, 2 * own), F32))
    pl.when(row > 0)(lambda: tail_copy().wait_recv())

    @pl.when(row == 0)
    def _():
        tail_in[...] = jnp.zeros_like(tail_in)

    before = tail_in[...]
    head = spans_at(0)
    nothing = jnp.zeros_like(before)
    left = jnp.concatenate([eig[:, :LANES], head], axis=0)
    acc = acc + dot_split(halves(left), halves(jnp.concatenate([before, nothing], axis=0)), LAST)
    tail = tail_out[...]
    beyond = dot_split(halves(tail), halves(jnp.concatenate([nothing, tail], axis=0)), LAST)
    pack[row, :columns, :] = acc[:columns]
    pack[row, columns : columns + own, :] = acc[columns:] + beyond
    pack[row, columns + own : columns + 2 * own, :] = dot_split(
        halves(before), halves(jnp.concatenate([head, nothing], axis=0)), LAST
    )

    def pack_copy(step):
        return pltpu.make_async_remote_copy(
            src_ref=pack.at[row], dst_ref=pack.at[row], send_sem=pack_send.at[step], recv_sem=pack_recv.at[row],
            device_id={"row": lax.rem(row + step, rows)}, device_id_type=pl.DeviceIdType.MESH,
        )

    def pack_taken(step):
        source = lax.rem(row + step, rows)
        return pltpu.make_async_remote_copy(
            src_ref=pack.at[source], dst_ref=pack.at[source], send_sem=pack_send.at[step], recv_sem=pack_recv.at[source],
            device_id={"row": source}, device_id_type=pl.DeviceIdType.MESH,
        )

    for step in range(1, rows):
        pack_copy(step).start()
    serve_all(0, 1) if line > 1 else None
    for step in range(1, rows):
        pack_taken(step).wait_recv()

    square = pack[0, columns + 2 * own :, :]
    for index in range(1, rows):
        square = square + pack[index, columns + 2 * own :, :]
    square = square[:, :width_own]
    down = lax.broadcasted_iota(jnp.int32, (width_own, width_own), 0)
    over = lax.broadcasted_iota(jnp.int32, (width_own, width_own), 1)
    square = jnp.where(down < over, square, jnp.where(down == over, 0.5 * square, 0.0))
    square = triangle_inverse(square, down, over, width_own)
    square = jnp.concatenate([square, jnp.zeros((width_own, LANES - width_own), F32)], axis=1)
    folded = square[:8]
    for index in range(1, fold):
        folded = folded + pltpu.roll(square[8 * index : 8 * index + 8], index * width_own, 1)
    corner[col] = folded

    def corner_copy(way, origin):
        return pltpu.make_async_remote_copy(
            src_ref=corner.at[origin], dst_ref=corner.at[origin],
            send_sem=corner_send.at[way, origin], recv_sem=corner_recv.at[origin],
            device_id=target(way), device_id_type=pl.DeviceIdType.MESH,
        )

    def send_corner(way, origin):
        def start():
            corner_copy(way, origin).start()

        if way == UP:
            pl.when(at < line - 1)(start)
        elif way == DOWN:
            pl.when(at > 0)(start)
        else:
            start()

    def serve_corner(step):
        for way, source in ((UP, at - step), (DOWN, at + step)):
            @pl.when((source >= 0) & (source < line))
            def _(way=way, source=source):
                origin = 2 * source + side
                corner_copy(way, origin).wait_recv()
                send_corner(way, origin)
                send_corner(ACROSS, origin)

    for way in (UP, DOWN, ACROSS):
        send_corner(way, col)

    def placed(value, shift):
        wide = value
        if total > 2 * own:
            zeros = jnp.zeros((value.shape[0], total - 2 * own), F32)
            wide = jnp.concatenate([value, zeros], axis=1)
        shift = shift * own % total
        return pltpu.roll(wide, shift, 1) if shift else wide

    inner = jnp.zeros((columns, total), F32)
    blocks = []
    for index in range(rows):
        inner = inner + placed(pack[index, :columns, :], index - 1)
        block = placed(pack[index, columns : columns + own, :], index - 1)
        if index < rows - 1:
            block = block + placed(pack[index + 1, columns + own : columns + 2 * own, :], index + 1)
        blocks.append(block)
    matrix = jnp.concatenate(blocks, axis=0)
    orders = []
    for axis in range(2):
        value = lax.broadcasted_iota(jnp.int32, (total, total), axis)
        part, within = value // own, value % own
        sweep_own = spans * refl
        orders.append((within // sweep_own) * (rows * sweep_own) + part * sweep_own + within % sweep_own)
    down, over = orders
    earlier = (down // refl > over // refl) | ((down // refl == over // refl) & (down < over))
    matrix = jnp.where(earlier, matrix, jnp.where(down == over, 0.5 * matrix, 0.0))
    coeffs = precise_dot(inner, triangle_inverse(matrix, down, over, total), LAST)
    coeffs = pltpu.roll(coeffs, lax.rem(total + own - own * row, total), 1)[:, : 2 * own]
    coeffs = halves(coeffs)
    for step in range(2, line - 1):
        serve_all(0, step)

    @pl.loop(0, groups)
    def _(index):
        spread = spans_group(index)
        right = jnp.concatenate([jnp.zeros_like(spread), spread], axis=0)
        eig[:, cut_group(index)] -= dot_split(coeffs, halves(right), INNER)

    eig[:, :LANES] -= dot_split(coeffs, halves(jnp.concatenate([before, nothing], axis=0)), INNER)
    if line > 2:
        serve_all(0, line - 1)
    serve_corner(1)
    for panel in range(1, panels):
        send_own(ACROSS, panel)

    def reflectors(panel, index, parts):
        return jnp.concatenate([walls[panel][part, :, cut(index)] for part in parts], axis=0)

    def rounded(index):
        return eig[:, cut(index)].astype(BF16)

    def row_copy(source, dest, send, recv, step):
        bit = 2**step
        low_bit = (row // bit) % 2
        return pltpu.make_async_remote_copy(
            src_ref=source, dst_ref=dest, send_sem=send, recv_sem=recv,
            device_id={"row": row + bit * (1 - 2 * low_bit)}, device_id_type=pl.DeviceIdType.MESH,
        )

    steps = rows.bit_length() - 1
    kept = (columns + width, columns + early_width)

    def row_sum(panel, meanwhile):
        rows_at = pl.ds(0, kept[panel])
        for step in range(steps):
            move = row_copy(
                sums.at[panel, rows_at], got.at[panel, step, rows_at],
                sum_send.at[panel, step], sum_recv.at[panel, step], step,
            )
            move.start()
            if step == steps - 1:
                meanwhile()
            move.wait()
            sums[panel, rows_at, :] += got[panel, step, rows_at, :]

    def triangle(gram):
        down = lax.broadcasted_iota(jnp.int32, (width, width), 0)
        over = lax.broadcasted_iota(jnp.int32, (width, width), 1)
        matrix = jnp.where(down < over, gram, jnp.where(down == over, 0.5 * gram, 0.0))
        return triangle_inverse(matrix, down, over, width)

    def diagonal(parts):
        stack = []
        for part in parts:
            folded = corner[part]
            stack.append(folded)
            for index in range(1, fold):
                stack.append(pltpu.roll(folded, LANES - index * width_own, 1))
        stack = jnp.concatenate(stack, axis=0)
        down = lax.broadcasted_iota(jnp.int32, (LANES, width), 0)
        over = lax.broadcasted_iota(jnp.int32, (LANES, width), 1) % width_own
        wide = precise_dot(stack, jnp.where(down == over, 1.0, 0.0).astype(F32))
        down = lax.broadcasted_iota(jnp.int32, (width, width), 0) // width_own
        over = lax.broadcasted_iota(jnp.int32, (width, width), 1) // width_own
        return jnp.where(down == over, wide, 0.0)

    def set_places(parts):
        for axis in range(2):
            part_at = lax.broadcasted_iota(jnp.int32, (width, width), axis) // width_own
            place = jnp.zeros_like(part_at)
            for index, part in enumerate(parts):
                place = jnp.where(part_at == index, part, place)
            places[axis] = place

    def solved(gram, inner, inverse):
        size = 1
        while size < cols:
            down, over = places[0], places[1]
            off = (down // (2 * size) == over // (2 * size)) & (down // size < over // size)
            off = halves(jnp.where(off, gram, 0.0))
            split = halves(inverse)
            inverse = inverse - dot_split(split, halves(dot_split(off, split, INNER)), INNER)
            size *= 2
        return dot_split(halves(inner), halves(inverse), LAST).astype(BF16)

    for panel in range(panels):
        sums[panel] = jnp.zeros_like(sums[panel])
    late[...] = jnp.zeros_like(late)
    natural = list(range(cols))

    @pl.loop(0, chunks)
    def _(index):
        for source in range(line):
            arrived(0, 2 * source + 1 - side, index)
        reflect = reflectors(0, index, natural)
        left = jnp.concatenate([rounded(index), reflect], axis=0)
        sums[0] += lax.dot_general(left, reflect, LAST, preferred_element_type=F32)
        serve(1, 1, index)

    def serve_between():
        for step in range(2, line - 1):
            @pl.loop(0, chunks)
            def _(index):
                serve(1, step, index)

        @pl.loop(0, chunks)
        def _(index):
            serve_partner(index)

    if line > 2:
        serve_corner(2)
    row_sum(0, serve_between)
    for step in range(3, line):
        serve_corner(step)
    coeffs = precise_dot(sums[0, :columns, :], triangle(sums[0, columns:, :]), LAST).astype(BF16)

    @pl.loop(0, chunks)
    def _(index):
        reflect = reflectors(0, index, natural)
        eig[:, cut(index)] -= lax.dot_general(coeffs, reflect, INNER, preferred_element_type=F32)

    early_parts, late_parts = order[:-2], order[-2:]

    @pl.loop(0, chunks)
    def _(index):
        serve(1, line - 1, index)
        for source in range(line):
            other = 2 * source + 1 - side
            known = (at == source) | (late_parts[0] == other) | (late_parts[1] == other)
            pl.when(jnp.logical_not(known))(lambda: arrived(1, other, index))
        reflect = reflectors(1, index, early_parts)
        left = jnp.concatenate([rounded(index), reflect], axis=0)
        right = jnp.concatenate([reflect, jnp.zeros((late_width, chunk), BF16)], axis=0)
        sums[1, pl.ds(0, kept[1]), :] += lax.dot_general(left, right, LAST, preferred_element_type=F32)

    def add_late(index):
        for part in late_parts:
            arrived(1, part, index)
        reflect = reflectors(1, index, late_parts)
        right = jnp.concatenate([reflectors(1, index, order), rounded(index)], axis=0)
        late[...] += lax.dot_general(reflect, right, LAST, preferred_element_type=F32)

    for source in range(line):
        corner_copy(ACROSS, 2 * source + 1 - side).wait_recv()
    set_places(order)
    row_sum(1, lambda: pl.loop(0, chunks - 1)(add_late))
    inverse = diagonal(order)
    add_late(chunks - 1)
    def gone(way, panel, origin):
        def wait():
            piece = walls[panel].at[origin]
            pltpu.make_async_remote_copy(
                src_ref=piece, dst_ref=piece, send_sem=send_sem.at[way, panel, origin],
                recv_sem=recv_sem.at[panel, origin, 0], device_id=target(way),
                device_id_type=pl.DeviceIdType.MESH,
            ).wait_send()

        if way == UP:
            pl.when(at < line - 1)(wait)
        elif way == DOWN:
            pl.when(at > 0)(wait)
        else:
            wait()

    def all_gone():
        for panel in range(panels):
            for source in range(line):
                origin = 2 * source + side
                pl.when(at >= source)(lambda: gone(UP, panel, origin))
                pl.when(at <= source)(lambda: gone(DOWN, panel, origin))
                pl.when(goes_across(panel, jnp.int32(source)))(lambda: gone(ACROSS, panel, origin))
        pl.when(at % 2 == 0)(lambda: gone(UP, last, 2 * at + 1 - side))
        pl.when(at % 2 == 1)(lambda: gone(DOWN, last, 2 * at + 1 - side))
        pl.when(row < rows - 1)(lambda: tail_copy().wait_send())
        for step in range(1, rows):
            pack_copy(step).wait_send()
        for source in range(line):
            origin = 2 * source + side
            pl.when((at >= source) & (at < line - 1))(lambda: corner_copy(UP, origin).wait_send())
            pl.when((at <= source) & (at > 0))(lambda: corner_copy(DOWN, origin).wait_send())
            corner_copy(ACROSS, origin).wait_send()

    for step in range(steps):
        move = row_copy(late, late_got.at[step], late_send.at[step], late_recv.at[step], step)
        move.start()
        if step == steps - 1:
            all_gone()
        move.wait()
        late[...] += late_got[step]
    down = lax.broadcasted_iota(jnp.int32, (late_width, width), 0)
    over = lax.broadcasted_iota(jnp.int32, (late_width, width), 1)
    turn = jnp.where(down + early_width == over, 1.0, 0.0).astype(F32)
    turned = precise_dot(late[...], turn, (((0,), (0,)), ((), ())))
    gram = jnp.concatenate(
        [sums[1, columns : columns + early_width, :] + turned[:early_width], late[:, :width]], axis=0
    )
    coef_ref[...] = solved(gram, sums[1, :columns, :] + turned[width:], inverse)


def finish_kernel(eig_ref, wall_ref, coef_ref, out_ref, held, sems):
    cols = wall_ref.shape[0]
    rows_dev = eig_ref.shape[1]
    chunk = tile_of(rows_dev, 14)
    chunks = rows_dev // chunk

    def cut(index):
        return pl.ds(pl.multiple_of(index * chunk, chunk), chunk)

    def copy(index):
        return pltpu.make_async_copy(held.at[:, cut(index)], out_ref.at[:, cut(index)], sems.at[index])

    coeffs = coef_ref[...]
    order = last_order(cols, lax.axis_index("col"))

    @pl.loop(0, chunks)
    def _(index):
        reflect = jnp.concatenate([wall_ref[part, :, cut(index)] for part in order], axis=0)
        update = lax.dot_general(coeffs, reflect, INNER, preferred_element_type=F32)
        held[:, cut(index)] = eig_ref[:, cut(index)] - update
        copy(index).start()

    @pl.loop(0, chunks)
    def _(index):
        copy(index).wait()


def local(eigvecs, span_vectors, span_offsets, panels):
    rows, cols = lax.axis_size("row"), lax.axis_size("col")
    columns, rows_dev = eigvecs.shape
    count, width_own, _ = panels.shape
    sweeps, spans, refl, band = span_vectors.shape
    own = sweeps * spans * refl
    width = width_own * cols
    steps = rows.bit_length() - 1
    chunks = rows_dev // tile_of(rows_dev, 14)
    late_width = 2 * width_own
    vmem = pltpu.VMEM
    dma = pltpu.SemaphoreType.DMA
    eigen, wall, coeffs = pl.pallas_call(
        kernel,
        out_shape=(
            vmem(eigvecs.shape, F32),
            vmem((cols, width_own, rows_dev), BF16),
            vmem((columns, width), BF16),
        ),
        in_specs=[pl.BlockSpec(memory_space=pltpu.HBM)] * 4,
        out_specs=[pl.BlockSpec(memory_space=pltpu.VMEM)] * 3,
        scratch_shapes=[
            vmem((cols, width_own, rows_dev), BF16),
            vmem(span_vectors.shape, F32),
            pltpu.SMEM(span_offsets.shape, jnp.int32),
            vmem((own, LANES), F32),
            vmem((own, LANES), F32),
            vmem((own, LANES), jnp.int32),
            vmem((own, LANES), F32),
            vmem((own, LANES), F32),
            vmem((rows, columns + 2 * own + width_own, 2 * own), F32),
            vmem((count, columns + width, width), F32),
            vmem((count, steps, columns + width, width), F32),
            vmem((late_width, columns + width), F32),
            vmem((steps, late_width, columns + width), F32),
            vmem((cols, 8, LANES), F32),
            vmem((2, width, width), jnp.int32),
            dma((3,)),
            dma((count,)),
            dma((count, cols, chunks)),
            dma((3, count, cols)),
            dma((2,)),
            dma((rows,)),
            dma((rows,)),
            dma((count, steps)),
            dma((count, steps)),
            dma((steps,)),
            dma((steps,)),
            dma((3, cols)),
            dma((cols,)),
        ],
        compiler_params=pltpu.CompilerParams(
            collective_id=0, has_side_effects=True, vmem_limit_bytes=40 * 2**20
        ),
        cost_estimate=pl.CostEstimate(
            flops=8 * width * (width + columns) * rows_dev,
            bytes_accessed=8 * rows_dev * columns + 8 * width * rows_dev,
            transcendentals=0,
        ),
    )(*(pltpu.with_memory_space_constraint(value, pltpu.HBM) for value in (eigvecs, span_vectors, span_offsets, panels)))
    return pl.pallas_call(
        finish_kernel,
        out_shape=jax.ShapeDtypeStruct(eigvecs.shape, F32),
        in_specs=[pl.BlockSpec(memory_space=pltpu.VMEM)] * 3,
        out_specs=pl.BlockSpec(memory_space=pl.ANY),
        scratch_shapes=[vmem(eigvecs.shape, F32), dma((chunks,))],
        compiler_params=pltpu.CompilerParams(vmem_limit_bytes=16 * 2**20),
        cost_estimate=pl.CostEstimate(
            flops=2 * width * columns * rows_dev, bytes_accessed=8 * columns * rows_dev, transcendentals=0
        ),
    )(eigen, wall, coeffs)


def solution(mesh):
    return jax.shard_map(
        local,
        mesh=mesh,
        in_specs=(
            P("col", "row"),
            P(None, "row", None, None),
            P(None, "row"),
            P(None, "col", "row"),
        ),
        out_specs=P("col", "row"),
        check_vma=False,
    )
```

```python
import functools

import jax
import jax.numpy as jnp
from jax import lax
from jax.experimental import pallas as pl
from jax.experimental.pallas import tpu as pltpu
from jax.sharding import PartitionSpec as P

PRECISE = lax.Precision.HIGHEST
LAST = (((1,), (1,)), ((), ()))
INNER = (((1,), (0,)), ((), ()))
LANES = 128
F32 = jnp.float32
BF16 = jnp.bfloat16
UP, DOWN, ACROSS = 0, 1, 2


def tile_of(rows_dev, most):
    count = rows_dev // LANES
    return LANES * max(part for part in range(1, most + 1) if count % part == 0)


def halves(value):
    high = value.astype(BF16)
    return high, (value - high.astype(F32)).astype(BF16)


def dot_split(left, right, dims):
    (left_high, left_low), (right_high, right_low) = left, right
    dot = functools.partial(lax.dot_general, dimension_numbers=dims, preferred_element_type=F32)
    return dot(left_high, right_high) + (dot(left_high, right_low) + dot(left_low, right_high))


def precise_dot(left, right, dims=INNER):
    return lax.dot_general(left, right, dims, precision=PRECISE, preferred_element_type=F32)


def triangle_inverse(matrix, down_at, across_at, order):
    same = down_at == across_at
    diagonal = jnp.where(same, matrix, 0.0)
    down = 1.0 / jnp.sum(diagonal, axis=1, keepdims=True)
    across = 1.0 / jnp.sum(diagonal, axis=0, keepdims=True)
    inverse = jnp.where(same, down, 0.0)
    beside = (down_at // 2 == across_at // 2) & (down_at != across_at)
    inverse = inverse - jnp.where(beside, matrix * down * across, 0.0)
    size = 2
    while size < order:
        together = down_at // (2 * size) == across_at // (2 * size)
        beside = together & (down_at // size != across_at // size)
        off = jnp.where(beside, matrix, 0.0)
        inverse = inverse - precise_dot(inverse, precise_dot(off, inverse))
        size *= 2
    return inverse


def natural_order(line):
    return [(side, place) for place in range(line) for side in range(2)]


def last_order(line, at, side):
    beside = at + 1 - 2 * (at % 2)
    far = (line - 1) * (1 - 2 * at // line)
    first, second = jnp.minimum(beside, far), jnp.maximum(beside, far)
    early = []
    for index in range(line - 2):
        place = index + jnp.where(first <= index, 1, 0)
        early.append(place + jnp.where(second <= place, 1, 0))
    order = [(side, place) for place in range(line)]
    return order + [(1 - side, place) for place in (*early, beside, far)]


def kernel(
    eig_ref, vec_ref, off_ref, pan_ref, eig, wall_last, coef_ref,
    wall_first, vecs, offs, low, high, base, tail_out, tail_in, pack, sums, got,
    late, late_got, late_cast, late_cast_got, corner, places, blocks,
    load_sem, own_sem, line_sem, first_sem, partner_sem, early_sem, last_sem, send_sem,
    tail_sem, pack_send, pack_recv, sum_send, sum_recv, late_send, late_recv,
    corner_send, corner_recv, corner_across,
):
    rows, cols = lax.axis_size("row"), lax.axis_size("col")
    line = cols // 2
    row, col = lax.axis_index("row"), lax.axis_index("col")
    at, side = col // 2, col % 2
    columns, rows_dev = eig.shape
    walls = (wall_first, wall_last)
    panels, width_own, _ = pan_ref.shape
    width = cols * width_own
    sweeps, spans, refl, band = vecs.shape
    own = sweeps * spans * refl
    total = rows * own
    chunk = tile_of(rows_dev, 14)
    chunks = rows_dev // chunk
    tiles = rows_dev // LANES
    group = tile_of(rows_dev, 7)
    groups = rows_dev // group
    last = panels - 1
    beside = at + 1 - 2 * (at % 2)
    far = (line - 1) * (1 - 2 * at // line)
    other = 1 - side
    natural, order = natural_order(line), last_order(line, at, side)
    late_width = 2 * width_own
    early_width = width - late_width
    fold = width_own // 8
    bounds = (0, (chunks + 1) // 2, chunks)

    def cut(index):
        return pl.ds(pl.multiple_of(index * chunk, chunk), chunk)

    short = max(1, chunk // LANES // 4) * LANES
    closing = (
        pl.ds(rows_dev - chunk, chunk - short),
        pl.ds(rows_dev - short, short),
    )

    def span_of(part):
        return pl.ds(bounds[part] * chunk, (bounds[part + 1] - bounds[part]) * chunk)

    def target(way):
        if way == ACROSS:
            return {"col": col + 1 - 2 * side}
        return {"col": col + 2 if way == UP else col - 2}

    def guarded(way, start):
        if way == UP:
            pl.when(at < line - 1)(start)
        elif way == DOWN:
            pl.when(at > 0)(start)
        else:
            start()

    def copy(way, panel, piece, where, sem, mine=False):
        dest = walls[panel].at[piece[0], piece[1], :, where]
        return pltpu.make_async_remote_copy(
            src_ref=pan_ref.at[panel, :, where] if mine else dest,
            dst_ref=dest,
            send_sem=send_sem.at[way, panel],
            recv_sem=sem,
            device_id=target(way),
            device_id_type=pl.DeviceIdType.MESH,
        )

    def send(way, panel, piece, where, sem, mine=False):
        guarded(way, lambda: copy(way, panel, piece, where, sem, mine).start())

    def arrived(panel, ref, sem):
        pltpu.make_async_remote_copy(
            src_ref=ref, dst_ref=ref, send_sem=send_sem.at[ACROSS, panel], recv_sem=sem,
            device_id=target(ACROSS), device_id_type=pl.DeviceIdType.MESH,
        ).wait_recv()

    def send_own(way, panel):
        for part in range(2):
            if way == ACROSS:
                sem = partner_sem.at[part] if panel == last else first_sem.at[part]
            else:
                sem = line_sem.at[panel, at, part]
            send(way, panel, (side, at), span_of(part), sem, True)

    def send_last(way, piece, part):
        @pl.loop(bounds[part], min(bounds[part + 1], chunks - 1))
        def _(index):
            send(way, last, piece, cut(index), last_sem.at[index])

        if bounds[part + 1] == chunks:
            for index, where in enumerate(closing):
                send(way, last, piece, where, last_sem.at[chunks - 1 + index])

    def serve(panel, step, part):
        for way, source in ((UP, at - step), (DOWN, at + step)):
            @pl.when((source >= 0) & (source < line))
            def _(way=way, source=source):
                piece = (side, source)
                sem = line_sem.at[panel, source, part]
                arrived(panel, walls[panel].at[side, source, :, span_of(part)], sem)
                send(way, panel, piece, span_of(part), sem)
                if panel < last:
                    send(ACROSS, panel, piece, span_of(part), first_sem.at[part])
                    return

                @pl.when(source == far)
                def _():
                    send_last(ACROSS, piece, part)

                @pl.when((source != far) & (source != beside))
                def _():
                    send(ACROSS, panel, piece, span_of(part), early_sem.at[part])

    def serve_all(panel, step):
        for part in range(2):
            serve(panel, step, part)
        if panel < last:
            @pl.when(at == step)
            def _():
                send_own(UP, panel + 1)

            @pl.when(at == line - 1 - step)
            def _():
                send_own(DOWN, panel + 1)

    def serve_partner(part):
        arrived(last, walls[last].at[other, at, :, span_of(part)], partner_sem.at[part])
        for way in (UP, DOWN):
            @pl.when(at % 2 == way)
            def _(way=way):
                send_last(way, (other, at), part)

    vec_load = pltpu.make_async_copy(vec_ref, vecs, load_sem.at[1])
    off_load = pltpu.make_async_copy(off_ref, offs, load_sem.at[2])
    vec_load.start()
    off_load.start()

    barrier = pltpu.get_barrier_semaphore()

    def greet(where):
        pl.semaphore_signal(barrier, inc=1, device_id=where, device_id_type=pl.DeviceIdType.MESH)

    greet(target(ACROSS))
    pl.when(at > 0)(lambda: greet(target(DOWN)))
    pl.when(at < line - 1)(lambda: greet(target(UP)))
    for step in range(1, rows):
        greet({"row": lax.rem(row + step, rows)})
    neighbours = jnp.minimum(at, 1) + jnp.minimum(line - 1 - at, 1)
    pl.semaphore_wait(barrier, rows + neighbours)

    send_own(UP, 0)
    send_own(DOWN, 0)
    send_own(ACROSS, 0)
    load = pltpu.make_async_copy(eig_ref, eig, load_sem.at[0])
    load.start()
    for panel in range(panels):
        pltpu.make_async_copy(pan_ref.at[panel], walls[panel].at[side, at], own_sem.at[panel]).start()
    pl.when(at == 0)(lambda: send_own(UP, 1))
    pl.when(at == line - 1)(lambda: send_own(DOWN, 1))

    vec_load.wait()
    off_load.wait()

    for index in range(sweeps * spans):
        low[index * refl : (index + 1) * refl, :] = vecs[index // spans, index % spans]
    per = 8 // refl
    for index in range(own // 8):
        rows_at = slice(8 * index, 8 * index + 8)
        spread = jnp.concatenate([low[rows_at, :], jnp.zeros((8, LANES), F32)], axis=1)
        moved = jnp.zeros_like(spread)
        first = jnp.zeros((8, LANES), jnp.int32)
        for part in range(per):
            span_at = index * per + part
            begin = offs[span_at // spans, span_at % spans]
            tile = begin // LANES
            turned = pltpu.roll(spread, begin - tile * LANES, 1)
            place = lax.broadcasted_iota(jnp.int32, (8, 2 * LANES), 0) // refl
            moved = jnp.where(place == part, turned, moved)
            first = jnp.where(place[:, :LANES] == part, tile, first)
        low[rows_at, :] = moved[:, :LANES]
        high[rows_at, :] = moved[:, LANES:]
        base[rows_at, :] = first

    def spans_at(tile):
        part = jnp.where(base[...] == tile, low[...], 0.0)
        return part + jnp.where(base[...] == tile - 1, high[...], 0.0)

    def spans_group(index):
        first = index * (group // LANES)
        return jnp.concatenate([spans_at(first + step) for step in range(group // LANES)], axis=1)

    def cut_group(index):
        return pl.ds(pl.multiple_of(index * group, group), group)

    tail_out[...] = jnp.where(base[...] == tiles - 1, high[...], 0.0)

    def tail_copy():
        return pltpu.make_async_remote_copy(
            src_ref=tail_out, dst_ref=tail_in, send_sem=tail_sem.at[0], recv_sem=tail_sem.at[1],
            device_id={"row": row + 1}, device_id_type=pl.DeviceIdType.MESH,
        )

    pl.when(row < rows - 1)(lambda: tail_copy().start())
    for panel in range(panels):
        pltpu.make_async_copy(pan_ref.at[panel], walls[panel].at[side, at], own_sem.at[panel]).wait()

    def own_products(index, acc):
        mine = walls[last][side, at, :, cut(index)]
        padded = jnp.concatenate([mine, jnp.zeros((LANES - width_own, chunk), BF16)], axis=0)
        return acc + lax.dot_general(mine, padded, LAST, preferred_element_type=F32)

    pack[row, columns + 2 * own :, :] = lax.fori_loop(0, chunks, own_products, jnp.zeros((width_own, LANES), F32))
    load.wait()

    def products(index, acc):
        spread = spans_group(index)
        left = jnp.concatenate([eig[:, cut_group(index)], spread], axis=0)
        right = jnp.concatenate([jnp.zeros_like(spread), spread], axis=0)
        return acc + dot_split(halves(left), halves(right), LAST)

    acc = lax.fori_loop(0, groups, products, jnp.zeros((columns + own, 2 * own), F32))
    pl.when(row > 0)(lambda: tail_copy().wait_recv())

    @pl.when(row == 0)
    def _():
        tail_in[...] = jnp.zeros_like(tail_in)

    before = tail_in[...]
    head = spans_at(0)
    nothing = jnp.zeros_like(before)
    left = jnp.concatenate([eig[:, :LANES], head], axis=0)
    acc = acc + dot_split(halves(left), halves(jnp.concatenate([before, nothing], axis=0)), LAST)
    tail = tail_out[...]
    beyond = dot_split(halves(tail), halves(jnp.concatenate([nothing, tail], axis=0)), LAST)
    pack[row, :columns, :] = acc[:columns]
    pack[row, columns : columns + own, :] = acc[columns:] + beyond
    pack[row, columns + own : columns + 2 * own, :] = dot_split(
        halves(before), halves(jnp.concatenate([head, nothing], axis=0)), LAST
    )

    def pack_copy(step):
        return pltpu.make_async_remote_copy(
            src_ref=pack.at[row], dst_ref=pack.at[row], send_sem=pack_send, recv_sem=pack_recv,
            device_id={"row": lax.rem(row + step, rows)}, device_id_type=pl.DeviceIdType.MESH,
        )

    def pack_others():
        ref = pack.at[pl.ds(0, rows - 1)]
        return pltpu.make_async_remote_copy(
            src_ref=ref, dst_ref=ref, send_sem=pack_send, recv_sem=pack_recv,
            device_id={"row": lax.rem(row + 1, rows)}, device_id_type=pl.DeviceIdType.MESH,
        )

    for step in range(1, rows):
        pack_copy(step).start()
    serve_all(0, 1)
    pack_others().wait_recv()

    square = pack[0, columns + 2 * own :, :]
    for index in range(1, rows):
        square = square + pack[index, columns + 2 * own :, :]
    square = square[:, :width_own]
    down = lax.broadcasted_iota(jnp.int32, (width_own, width_own), 0)
    over = lax.broadcasted_iota(jnp.int32, (width_own, width_own), 1)
    square = jnp.where(down < over, square, jnp.where(down == over, 0.5 * square, 0.0))
    square = triangle_inverse(square, down, over, width_own)
    square = jnp.concatenate([square, jnp.zeros((width_own, LANES - width_own), F32)], axis=1)
    folded = square[:8]
    for index in range(1, fold):
        folded = folded + pltpu.roll(square[8 * index : 8 * index + 8], index * width_own, 1)
    corner[side, at] = folded

    def send_corner(way, source):
        ref = corner.at[side, source]
        move = pltpu.make_async_remote_copy(
            src_ref=ref, dst_ref=ref, send_sem=corner_send.at[way],
            recv_sem=corner_across if way == ACROSS else corner_recv.at[source],
            device_id=target(way), device_id_type=pl.DeviceIdType.MESH,
        )
        guarded(way, move.start)

    def corner_wait(ref, way, sem):
        return pltpu.make_async_remote_copy(
            src_ref=ref, dst_ref=ref, send_sem=corner_send.at[way], recv_sem=sem,
            device_id=target(way), device_id_type=pl.DeviceIdType.MESH,
        )

    def serve_corner(step):
        for way, source in ((UP, at - step), (DOWN, at + step)):
            @pl.when((source >= 0) & (source < line))
            def _(way=way, source=source):
                corner_wait(corner.at[side, source], ACROSS, corner_recv.at[source]).wait_recv()
                send_corner(way, source)
                send_corner(ACROSS, source)

    for way in (UP, DOWN, ACROSS):
        send_corner(way, at)

    def placed(value, shift):
        wide = value
        if total > 2 * own:
            zeros = jnp.zeros((value.shape[0], total - 2 * own), F32)
            wide = jnp.concatenate([value, zeros], axis=1)
        shift = shift * own % total
        return pltpu.roll(wide, shift, 1) if shift else wide

    inner = jnp.zeros((columns, total), F32)
    bands = []
    for index in range(rows):
        inner = inner + placed(pack[index, :columns, :], index - 1)
        block = placed(pack[index, columns : columns + own, :], index - 1)
        if index < rows - 1:
            block = block + placed(pack[index + 1, columns + own : columns + 2 * own, :], index + 1)
        bands.append(block)
    matrix = jnp.concatenate(bands, axis=0)
    orders = []
    for axis in range(2):
        value = lax.broadcasted_iota(jnp.int32, (total, total), axis)
        part, within = value // own, value % own
        sweep_own = spans * refl
        orders.append((within // sweep_own) * (rows * sweep_own) + part * sweep_own + within % sweep_own)
    down, over = orders
    earlier = (down // refl > over // refl) | ((down // refl == over // refl) & (down < over))
    matrix = jnp.where(earlier, matrix, jnp.where(down == over, 0.5 * matrix, 0.0))
    coeffs = precise_dot(inner, triangle_inverse(matrix, down, over, total), LAST)
    coeffs = pltpu.roll(coeffs, lax.rem(total + own - own * row, total), 1)[:, : 2 * own]
    coeffs = halves(coeffs)
    for step in range(2, line - 1):
        serve_all(0, step)

    @pl.loop(0, groups)
    def _(index):
        spread = spans_group(index)
        right = jnp.concatenate([jnp.zeros_like(spread), spread], axis=0)
        eig[:, cut_group(index)] -= dot_split(coeffs, halves(right), INNER)

    eig[:, :LANES] -= dot_split(coeffs, halves(jnp.concatenate([before, nothing], axis=0)), INNER)
    serve_all(0, line - 1)
    serve_corner(1)
    for panel in range(1, panels):
        send_own(ACROSS, panel)

    def reflectors(panel, where, parts):
        return jnp.concatenate([walls[panel][part[0], part[1], :, where] for part in parts], axis=0)

    def rounded(where):
        return eig[:, where].astype(BF16)

    def row_copy(source, dest, send, recv, step):
        bit = 2**step
        low_bit = (row // bit) % 2
        return pltpu.make_async_remote_copy(
            src_ref=source, dst_ref=dest, send_sem=send, recv_sem=recv,
            device_id={"row": row + bit * (1 - 2 * low_bit)}, device_id_type=pl.DeviceIdType.MESH,
        )

    steps = rows.bit_length() - 1
    kept = (columns + width, columns + early_width)

    def row_sum(panel, meanwhile):
        rows_at = pl.ds(0, kept[panel])
        for step in range(steps):
            move = row_copy(
                sums.at[panel, rows_at], got.at[panel, step, rows_at],
                sum_send.at[panel, step], sum_recv.at[panel, step], step,
            )
            move.start()
            if step == steps - 1:
                meanwhile()
            move.wait()
            sums[panel, rows_at, :] += got[panel, step, rows_at, :]

    def triangle(gram):
        down = lax.broadcasted_iota(jnp.int32, (width, width), 0)
        over = lax.broadcasted_iota(jnp.int32, (width, width), 1)
        matrix = jnp.where(down < over, gram, jnp.where(down == over, 0.5 * gram, 0.0))
        return triangle_inverse(matrix, down, over, width)

    def diagonal(parts):
        stack = []
        for part in parts:
            folded = corner[part[0], part[1]]
            stack.append(folded)
            for index in range(1, fold):
                stack.append(pltpu.roll(folded, LANES - index * width_own, 1))
        stack = jnp.concatenate(stack, axis=0)
        down = lax.broadcasted_iota(jnp.int32, (LANES, width), 0)
        over = lax.broadcasted_iota(jnp.int32, (LANES, width), 1) % width_own
        wide = precise_dot(stack, jnp.where(down == over, 1.0, 0.0).astype(F32))
        down = lax.broadcasted_iota(jnp.int32, (width, width), 0) // width_own
        over = lax.broadcasted_iota(jnp.int32, (width, width), 1) // width_own
        return jnp.where(down == over, wide, 0.0)

    def set_places(parts):
        for axis in range(2):
            part_at = lax.broadcasted_iota(jnp.int32, (width, width), axis) // width_own
            place = jnp.zeros_like(part_at)
            for index, part in enumerate(parts):
                place = jnp.where(part_at == index, 2 * part[1] + part[0], place)
            places[axis] = place

    def solved(gram, inner, inverse):
        down, over = places[0], places[1]
        if cols > 8:
            size = 1
            while size < cols:
                off = (down // (2 * size) == over // (2 * size)) & (down // size < over // size)
                off = halves(jnp.where(off, gram, 0.0))
                split = halves(inverse)
                inverse = inverse - dot_split(split, halves(dot_split(off, split, INNER)), INNER)
                size *= 2
            return dot_split(halves(inner), halves(inverse), LAST).astype(BF16)
        split = halves(inverse)
        power = halves(dot_split(split, halves(jnp.where(down < over, gram, 0.0)), INNER))
        value = dot_split(halves(inner), split, LAST)
        value = value - dot_split(halves(value), power, LAST)
        size = 2
        while size < cols:
            power = halves(dot_split(power, power, INNER))
            value = value + dot_split(halves(value), power, LAST)
            size *= 2
        return value.astype(BF16)

    for panel in range(panels):
        sums[panel] = jnp.zeros_like(sums[panel])
    late[...] = jnp.zeros_like(late)
    for part in range(2):
        arrived(0, walls[0].at[other, :, :, span_of(part)], first_sem.at[part])

        @pl.loop(bounds[part], bounds[part + 1])
        def _(index):
            reflect = reflectors(0, cut(index), natural)
            left = jnp.concatenate([rounded(cut(index)), reflect], axis=0)
            sums[0] += lax.dot_general(left, reflect, LAST, preferred_element_type=F32)

        serve(1, 1, part)

    def serve_between():
        for step in range(2, line - 1):
            for part in range(2):
                serve(1, step, part)
        for part in range(2):
            serve_partner(part)

    serve_corner(2)
    row_sum(0, serve_between)
    for step in range(3, line):
        serve_corner(step)
    coeffs = precise_dot(sums[0, :columns, :], triangle(sums[0, columns:, :]), LAST).astype(BF16)

    @pl.loop(0, chunks)
    def _(index):
        reflect = reflectors(0, cut(index), natural)
        eig[:, cut(index)] -= lax.dot_general(coeffs, reflect, INNER, preferred_element_type=F32)

    early_parts, late_parts = order[:-2], order[-2:]

    for part in range(2):
        serve(1, line - 1, part)
        arrived(1, walls[1].at[other, pl.ds(0, line - 3), :, span_of(part)], early_sem.at[part])

        @pl.loop(bounds[part], bounds[part + 1])
        def _(index):
            reflect = reflectors(1, cut(index), early_parts)
            left = jnp.concatenate([rounded(cut(index)), reflect], axis=0)
            right = jnp.concatenate([reflect, jnp.zeros((late_width, chunk), BF16)], axis=0)
            sums[1, pl.ds(0, kept[1]), :] += lax.dot_general(left, right, LAST, preferred_element_type=F32)

    def add_late(where, sem):
        arrived(1, walls[1].at[other, pl.ds(0, 2), :, where], sem)
        reflect = reflectors(1, where, late_parts)
        right = jnp.concatenate([reflectors(1, where, order), rounded(where)], axis=0)
        late[...] += lax.dot_general(reflect, right, LAST, preferred_element_type=F32)

    def prepare():
        corner_wait(corner.at[other], ACROSS, corner_across).wait_recv()
        set_places(order)
        blocks[...] = diagonal(order)
        pl.loop(0, max(chunks - 2, 0))(lambda index: add_late(cut(index), last_sem.at[index]))

    row_sum(1, prepare)
    for index in range(max(chunks - 2, 0), chunks - 1):
        add_late(cut(index), last_sem.at[index])
    for index, where in enumerate(closing):
        add_late(where, last_sem.at[chunks - 1 + index])

    def gone(ref, way, sem):
        pltpu.make_async_remote_copy(
            src_ref=ref, dst_ref=ref, send_sem=sem, recv_sem=partner_sem.at[0], device_id=target(way),
            device_id_type=pl.DeviceIdType.MESH,
        ).wait_send()

    def all_gone():
        for panel in range(panels):
            pieces = walls[panel].at[0]
            for place in range(line):
                @pl.when(at == place)
                def _(place=place):
                    above, below = place + 1, line - place
                    if panel == last:
                        above, below = above + 1 - place % 2, below + place % 2
                    if place < line - 1:
                        gone(pieces.at[pl.ds(0, above)], UP, send_sem.at[UP, panel])
                    if place > 0:
                        gone(pieces.at[pl.ds(0, below)], DOWN, send_sem.at[DOWN, panel])
            count = line - 1 if panel == last else line
            gone(pieces.at[pl.ds(0, count)], ACROSS, send_sem.at[ACROSS, panel])
        for place in range(line):
            @pl.when(at == place)
            def _(place=place):
                if place < line - 1:
                    corner_wait(corner.at[0, pl.ds(0, place + 1)], UP, corner_across).wait_send()
                if place > 0:
                    corner_wait(corner.at[0, pl.ds(0, line - place)], DOWN, corner_across).wait_send()
        corner_wait(corner.at[0], ACROSS, corner_across).wait_send()
        pl.when(row < rows - 1)(lambda: tail_copy().wait_send())
        pack_others().wait_send()

    for step in range(steps):
        if step == 0:
            move = row_copy(late, late_got, late_send.at[step], late_recv.at[step], step)
        else:
            late_cast[...] = late[...].astype(BF16)
            move = row_copy(late_cast, late_cast_got.at[step - 1], late_send.at[step], late_recv.at[step], step)
        move.start()
        if step == steps - 1:
            all_gone()
        move.wait()
        late[...] += late_got[...] if step == 0 else late_cast_got[step - 1].astype(F32)
    down = lax.broadcasted_iota(jnp.int32, (late_width, width), 0)
    over = lax.broadcasted_iota(jnp.int32, (late_width, width), 1)
    turn = jnp.where(down + early_width == over, 1.0, 0.0).astype(BF16)
    first_dim = (((0,), (0,)), ((), ()))
    turned = sum(lax.dot_general(part, turn, first_dim, preferred_element_type=F32) for part in halves(late[...]))
    gram = jnp.concatenate(
        [sums[1, columns : columns + early_width, :] + turned[:early_width], late[:, :width]], axis=0
    )
    coef_ref[...] = solved(gram, sums[1, :columns, :] + turned[width:], blocks[...])


def finish_kernel(eig_ref, wall_ref, coef_ref, out_ref, held, sems):
    line = wall_ref.shape[1]
    rows_dev = eig_ref.shape[1]
    chunk = tile_of(rows_dev, 14)
    chunks = rows_dev // chunk

    def cut(index):
        return pl.ds(pl.multiple_of(index * chunk, chunk), chunk)

    def copy(index):
        return pltpu.make_async_copy(held.at[:, cut(index)], out_ref.at[:, cut(index)], sems.at[index])

    coeffs = coef_ref[...]
    col = lax.axis_index("col")
    order = last_order(line, col // 2, col % 2)

    for index in range(chunks):
        reflect = jnp.concatenate([wall_ref[part[0], part[1], :, cut(index)] for part in order], axis=0)
        update = lax.dot_general(coeffs, reflect, INNER, preferred_element_type=F32)
        held[:, cut(index)] = eig_ref[:, cut(index)] - update
        copy(index).start()

    @pl.loop(0, chunks)
    def _(index):
        copy(index).wait()


def local(eigvecs, span_vectors, span_offsets, panels):
    rows, cols = lax.axis_size("row"), lax.axis_size("col")
    columns, rows_dev = eigvecs.shape
    count, width_own, _ = panels.shape
    sweeps, spans, refl, band = span_vectors.shape
    own = sweeps * spans * refl
    width = width_own * cols
    steps = rows.bit_length() - 1
    chunks = rows_dev // tile_of(rows_dev, 14)
    late_width = 2 * width_own
    line = cols // 2
    vmem = pltpu.VMEM
    dma = pltpu.SemaphoreType.DMA
    eigen, wall, coeffs = pl.pallas_call(
        kernel,
        out_shape=(
            vmem(eigvecs.shape, F32),
            vmem((2, line, width_own, rows_dev), BF16),
            vmem((columns, width), BF16),
        ),
        in_specs=[pl.BlockSpec(memory_space=pltpu.HBM)] * 4,
        out_specs=[pl.BlockSpec(memory_space=pltpu.VMEM)] * 3,
        scratch_shapes=[
            vmem((2, line, width_own, rows_dev), BF16),
            vmem(span_vectors.shape, F32),
            pltpu.SMEM(span_offsets.shape, jnp.int32),
            vmem((own, LANES), F32),
            vmem((own, LANES), F32),
            vmem((own, LANES), jnp.int32),
            vmem((own, LANES), F32),
            vmem((own, LANES), F32),
            vmem((rows, columns + 2 * own + width_own, 2 * own), F32),
            vmem((count, columns + width, width), F32),
            vmem((count, steps, columns + width, width), F32),
            vmem((late_width, columns + width), F32),
            vmem((late_width, columns + width), F32),
            vmem((late_width, columns + width), BF16),
            vmem((steps, late_width, columns + width), BF16),
            vmem((2, line, 8, LANES), F32),
            vmem((2, width, width), jnp.int32),
            vmem((width, width), F32),
            dma((3,)),
            dma((count,)),
            dma((count, line, 2)),
            dma((2,)),
            dma((2,)),
            dma((2,)),
            dma((chunks + 1,)),
            dma((3, count)),
            dma((2,)),
            dma,
            dma,
            dma((count, steps)),
            dma((count, steps)),
            dma((steps,)),
            dma((steps,)),
            dma((3,)),
            dma((line,)),
            dma,
        ],
        compiler_params=pltpu.CompilerParams(
            collective_id=0, has_side_effects=True, vmem_limit_bytes=40 * 2**20
        ),
        cost_estimate=pl.CostEstimate(
            flops=8 * width * (width + columns) * rows_dev,
            bytes_accessed=8 * rows_dev * columns + 8 * width * rows_dev,
            transcendentals=0,
        ),
    )(*(pltpu.with_memory_space_constraint(value, pltpu.HBM) for value in (eigvecs, span_vectors, span_offsets, panels)))
    return pl.pallas_call(
        finish_kernel,
        out_shape=jax.ShapeDtypeStruct(eigvecs.shape, F32),
        in_specs=[pl.BlockSpec(memory_space=pltpu.VMEM)] * 3,
        out_specs=pl.BlockSpec(memory_space=pl.ANY),
        scratch_shapes=[vmem(eigvecs.shape, F32), dma((rows_dev // tile_of(rows_dev, 14),))],
        compiler_params=pltpu.CompilerParams(vmem_limit_bytes=16 * 2**20),
        cost_estimate=pl.CostEstimate(
            flops=2 * width * columns * rows_dev, bytes_accessed=8 * columns * rows_dev, transcendentals=0
        ),
    )(eigen, wall, coeffs)


def solution(mesh):
    return jax.shard_map(
        local,
        mesh=mesh,
        in_specs=(
            P("col", "row"),
            P(None, "row", None, None),
            P(None, "row"),
            P(None, "col", "row"),
        ),
        out_specs=P("col", "row"),
        check_vma=False,
    )
```

```python
import functools

import jax
import jax.numpy as jnp
from jax import lax
from jax.experimental import pallas as pl
from jax.experimental.pallas import tpu as pltpu
from jax.sharding import PartitionSpec as P

PRECISE = lax.Precision.HIGHEST
LAST = (((1,), (1,)), ((), ()))
INNER = (((1,), (0,)), ((), ()))
LANES = 128
F32 = jnp.float32
BF16 = jnp.bfloat16
UP, DOWN, ACROSS = 0, 1, 2


def tile_of(rows_dev, most):
    count = rows_dev // LANES
    return LANES * max(part for part in range(1, most + 1) if count % part == 0)


def halves(value):
    high = value.astype(BF16)
    return high, (value - high.astype(F32)).astype(BF16)


def dot_split(left, right, dims):
    (left_high, left_low), (right_high, right_low) = left, right
    dot = functools.partial(lax.dot_general, dimension_numbers=dims, preferred_element_type=F32)
    return dot(left_high, right_high) + (dot(left_high, right_low) + dot(left_low, right_high))


def precise_dot(left, right, dims=INNER):
    return lax.dot_general(left, right, dims, precision=PRECISE, preferred_element_type=F32)


def triangle_inverse(matrix, down_at, across_at, order):
    same = down_at == across_at
    diagonal = jnp.where(same, matrix, 0.0)
    down = 1.0 / jnp.sum(diagonal, axis=1, keepdims=True)
    across = 1.0 / jnp.sum(diagonal, axis=0, keepdims=True)
    inverse = jnp.where(same, down, 0.0)
    beside = (down_at // 2 == across_at // 2) & (down_at != across_at)
    inverse = inverse - jnp.where(beside, matrix * down * across, 0.0)
    size = 2
    while size < order:
        together = down_at // (2 * size) == across_at // (2 * size)
        beside = together & (down_at // size != across_at // size)
        off = jnp.where(beside, matrix, 0.0)
        inverse = inverse - precise_dot(inverse, precise_dot(off, inverse))
        size *= 2
    return inverse


def natural_order(line):
    return [(side, place) for place in range(line) for side in range(2)]


def last_order(line, at, side):
    beside = at + 1 - 2 * (at % 2)
    far = (line - 1) * (1 - 2 * at // line)
    first, second = jnp.minimum(beside, far), jnp.maximum(beside, far)
    early = []
    for index in range(line - 2):
        place = index + jnp.where(first <= index, 1, 0)
        early.append(place + jnp.where(second <= place, 1, 0))
    order = [(side, place) for place in range(line)]
    return order + [(1 - side, place) for place in (*early, beside, far)]


def kernel(
    eig_ref, vec_ref, off_ref, pan_ref, eig, wall_last, coef_ref,
    wall_first, vecs, offs, low, high, base, tail_out, tail_in, pack, sums, got,
    late, late_got, late_cast, late_cast_got, bulk, bulk_got, corner, places, blocks,
    load_sem, own_sem, line_sem, first_sem, partner_sem, early_sem, last_sem, send_sem,
    tail_sem, pack_send, pack_recv, sum_send, sum_recv, late_send, late_recv,
    bulk_send, bulk_recv, corner_send, corner_recv, corner_across,
):
    rows, cols = lax.axis_size("row"), lax.axis_size("col")
    line = cols // 2
    row, col = lax.axis_index("row"), lax.axis_index("col")
    at, side = col // 2, col % 2
    columns, rows_dev = eig.shape
    walls = (wall_first, wall_last)
    panels, width_own, _ = pan_ref.shape
    width = cols * width_own
    sweeps, spans, refl, band = vecs.shape
    own = sweeps * spans * refl
    total = rows * own
    chunk = tile_of(rows_dev, 14)
    chunks = rows_dev // chunk
    tiles = rows_dev // LANES
    group = tile_of(rows_dev, 7)
    groups = rows_dev // group
    last = panels - 1
    beside = at + 1 - 2 * (at % 2)
    far = (line - 1) * (1 - 2 * at // line)
    other = 1 - side
    natural, order = natural_order(line), last_order(line, at, side)
    late_width = 2 * width_own
    early_width = width - late_width
    fold = width_own // 8
    bounds = (0, (chunks + 1) // 2, chunks)

    def cut(index):
        return pl.ds(pl.multiple_of(index * chunk, chunk), chunk)

    short = max(1, chunk // LANES // 4) * LANES
    closing = (
        pl.ds(rows_dev - chunk, chunk - short),
        pl.ds(rows_dev - short, short),
    )

    def span_of(part):
        return pl.ds(bounds[part] * chunk, (bounds[part + 1] - bounds[part]) * chunk)

    def target(way):
        if way == ACROSS:
            return {"col": col + 1 - 2 * side}
        return {"col": col + 2 if way == UP else col - 2}

    def guarded(way, start):
        if way == UP:
            pl.when(at < line - 1)(start)
        elif way == DOWN:
            pl.when(at > 0)(start)
        else:
            start()

    def copy(way, panel, piece, where, sem, mine=False):
        dest = walls[panel].at[piece[0], piece[1], :, where]
        return pltpu.make_async_remote_copy(
            src_ref=pan_ref.at[panel, :, where] if mine else dest,
            dst_ref=dest,
            send_sem=send_sem.at[way, panel],
            recv_sem=sem,
            device_id=target(way),
            device_id_type=pl.DeviceIdType.MESH,
        )

    def send(way, panel, piece, where, sem, mine=False):
        guarded(way, lambda: copy(way, panel, piece, where, sem, mine).start())

    def arrived(panel, ref, sem):
        pltpu.make_async_remote_copy(
            src_ref=ref, dst_ref=ref, send_sem=send_sem.at[ACROSS, panel], recv_sem=sem,
            device_id=target(ACROSS), device_id_type=pl.DeviceIdType.MESH,
        ).wait_recv()

    def send_own(way, panel):
        for part in range(2):
            if way == ACROSS:
                sem = partner_sem.at[part] if panel == last else first_sem.at[part]
            else:
                sem = line_sem.at[panel, at, part]
            send(way, panel, (side, at), span_of(part), sem, True)

    def send_last(way, piece, part):
        @pl.loop(bounds[part], min(bounds[part + 1], chunks - 1))
        def _(index):
            send(way, last, piece, cut(index), last_sem.at[index])

        if bounds[part + 1] == chunks:
            for index, where in enumerate(closing):
                send(way, last, piece, where, last_sem.at[chunks - 1 + index])

    def serve(panel, step, part):
        for way, source in ((UP, at - step), (DOWN, at + step)):
            @pl.when((source >= 0) & (source < line))
            def _(way=way, source=source):
                piece = (side, source)
                sem = line_sem.at[panel, source, part]
                arrived(panel, walls[panel].at[side, source, :, span_of(part)], sem)
                send(way, panel, piece, span_of(part), sem)
                if panel < last:
                    send(ACROSS, panel, piece, span_of(part), first_sem.at[part])
                    return

                @pl.when(source == far)
                def _():
                    send_last(ACROSS, piece, part)

                @pl.when((source != far) & (source != beside))
                def _():
                    send(ACROSS, panel, piece, span_of(part), early_sem.at[part])

    def serve_all(panel, step):
        for part in range(2):
            serve(panel, step, part)
        if panel < last:
            @pl.when(at == step)
            def _():
                send_own(UP, panel + 1)

            @pl.when(at == line - 1 - step)
            def _():
                send_own(DOWN, panel + 1)

    def serve_partner(part):
        arrived(last, walls[last].at[other, at, :, span_of(part)], partner_sem.at[part])
        for way in (UP, DOWN):
            @pl.when(at % 2 == way)
            def _(way=way):
                send_last(way, (other, at), part)

    vec_load = pltpu.make_async_copy(vec_ref, vecs, load_sem.at[1])
    off_load = pltpu.make_async_copy(off_ref, offs, load_sem.at[2])
    vec_load.start()
    off_load.start()

    barrier = pltpu.get_barrier_semaphore()

    def greet(where):
        pl.semaphore_signal(barrier, inc=1, device_id=where, device_id_type=pl.DeviceIdType.MESH)

    greet(target(ACROSS))
    pl.when(at > 0)(lambda: greet(target(DOWN)))
    pl.when(at < line - 1)(lambda: greet(target(UP)))
    for step in range(1, rows):
        greet({"row": lax.rem(row + step, rows)})
    neighbours = jnp.minimum(at, 1) + jnp.minimum(line - 1 - at, 1)
    pl.semaphore_wait(barrier, rows + neighbours)

    send_own(UP, 0)
    send_own(DOWN, 0)
    send_own(ACROSS, 0)
    load = pltpu.make_async_copy(eig_ref, eig, load_sem.at[0])
    load.start()
    for panel in range(panels):
        pltpu.make_async_copy(pan_ref.at[panel], walls[panel].at[side, at], own_sem.at[panel]).start()
    pl.when(at == 0)(lambda: send_own(UP, 1))
    pl.when(at == line - 1)(lambda: send_own(DOWN, 1))

    vec_load.wait()
    off_load.wait()

    for index in range(sweeps * spans):
        low[index * refl : (index + 1) * refl, :] = vecs[index // spans, index % spans]
    per = 8 // refl
    for index in range(own // 8):
        rows_at = slice(8 * index, 8 * index + 8)
        spread = jnp.concatenate([low[rows_at, :], jnp.zeros((8, LANES), F32)], axis=1)
        moved = jnp.zeros_like(spread)
        first = jnp.zeros((8, LANES), jnp.int32)
        for part in range(per):
            span_at = index * per + part
            begin = offs[span_at // spans, span_at % spans]
            tile = begin // LANES
            turned = pltpu.roll(spread, begin - tile * LANES, 1)
            place = lax.broadcasted_iota(jnp.int32, (8, 2 * LANES), 0) // refl
            moved = jnp.where(place == part, turned, moved)
            first = jnp.where(place[:, :LANES] == part, tile, first)
        low[rows_at, :] = moved[:, :LANES]
        high[rows_at, :] = moved[:, LANES:]
        base[rows_at, :] = first

    def spans_at(tile):
        part = jnp.where(base[...] == tile, low[...], 0.0)
        return part + jnp.where(base[...] == tile - 1, high[...], 0.0)

    def spans_group(index):
        first = index * (group // LANES)
        return jnp.concatenate([spans_at(first + step) for step in range(group // LANES)], axis=1)

    def cut_group(index):
        return pl.ds(pl.multiple_of(index * group, group), group)

    tail_out[...] = jnp.where(base[...] == tiles - 1, high[...], 0.0)

    def tail_copy():
        return pltpu.make_async_remote_copy(
            src_ref=tail_out, dst_ref=tail_in, send_sem=tail_sem.at[0], recv_sem=tail_sem.at[1],
            device_id={"row": row + 1}, device_id_type=pl.DeviceIdType.MESH,
        )

    pl.when(row < rows - 1)(lambda: tail_copy().start())
    for panel in range(panels):
        pltpu.make_async_copy(pan_ref.at[panel], walls[panel].at[side, at], own_sem.at[panel]).wait()

    def own_products(index, acc):
        mine = walls[last][side, at, :, cut(index)]
        padded = jnp.concatenate([mine, jnp.zeros((LANES - width_own, chunk), BF16)], axis=0)
        return acc + lax.dot_general(mine, padded, LAST, preferred_element_type=F32)

    pack[row, columns + 2 * own :, :] = lax.fori_loop(0, chunks, own_products, jnp.zeros((width_own, LANES), F32))
    load.wait()

    def products(index, acc):
        spread = spans_group(index)
        left = jnp.concatenate([eig[:, cut_group(index)], spread], axis=0)
        right = jnp.concatenate([jnp.zeros_like(spread), spread], axis=0)
        return acc + dot_split(halves(left), halves(right), LAST)

    acc = lax.fori_loop(0, groups, products, jnp.zeros((columns + own, 2 * own), F32))
    pl.when(row > 0)(lambda: tail_copy().wait_recv())

    @pl.when(row == 0)
    def _():
        tail_in[...] = jnp.zeros_like(tail_in)

    before = tail_in[...]
    head = spans_at(0)
    nothing = jnp.zeros_like(before)
    left = jnp.concatenate([eig[:, :LANES], head], axis=0)
    acc = acc + dot_split(halves(left), halves(jnp.concatenate([before, nothing], axis=0)), LAST)
    tail = tail_out[...]
    beyond = dot_split(halves(tail), halves(jnp.concatenate([nothing, tail], axis=0)), LAST)
    pack[row, :columns, :] = acc[:columns]
    pack[row, columns : columns + own, :] = acc[columns:] + beyond
    pack[row, columns + own : columns + 2 * own, :] = dot_split(
        halves(before), halves(jnp.concatenate([head, nothing], axis=0)), LAST
    )

    def pack_copy(step):
        return pltpu.make_async_remote_copy(
            src_ref=pack.at[row], dst_ref=pack.at[row], send_sem=pack_send, recv_sem=pack_recv,
            device_id={"row": lax.rem(row + step, rows)}, device_id_type=pl.DeviceIdType.MESH,
        )

    def pack_others():
        ref = pack.at[pl.ds(0, rows - 1)]
        return pltpu.make_async_remote_copy(
            src_ref=ref, dst_ref=ref, send_sem=pack_send, recv_sem=pack_recv,
            device_id={"row": lax.rem(row + 1, rows)}, device_id_type=pl.DeviceIdType.MESH,
        )

    for step in range(1, rows):
        pack_copy(step).start()
    serve_all(0, 1)
    pack_others().wait_recv()

    square = pack[0, columns + 2 * own :, :]
    for index in range(1, rows):
        square = square + pack[index, columns + 2 * own :, :]
    square = square[:, :width_own]
    down = lax.broadcasted_iota(jnp.int32, (width_own, width_own), 0)
    over = lax.broadcasted_iota(jnp.int32, (width_own, width_own), 1)
    square = jnp.where(down < over, square, jnp.where(down == over, 0.5 * square, 0.0))
    square = triangle_inverse(square, down, over, width_own)
    square = jnp.concatenate([square, jnp.zeros((width_own, LANES - width_own), F32)], axis=1)
    folded = square[:8]
    for index in range(1, fold):
        folded = folded + pltpu.roll(square[8 * index : 8 * index + 8], index * width_own, 1)
    corner[side, at] = folded

    def send_corner(way, source):
        ref = corner.at[side, source]
        move = pltpu.make_async_remote_copy(
            src_ref=ref, dst_ref=ref, send_sem=corner_send.at[way],
            recv_sem=corner_across if way == ACROSS else corner_recv.at[source],
            device_id=target(way), device_id_type=pl.DeviceIdType.MESH,
        )
        guarded(way, move.start)

    def corner_wait(ref, way, sem):
        return pltpu.make_async_remote_copy(
            src_ref=ref, dst_ref=ref, send_sem=corner_send.at[way], recv_sem=sem,
            device_id=target(way), device_id_type=pl.DeviceIdType.MESH,
        )

    def serve_corner(step):
        for way, source in ((UP, at - step), (DOWN, at + step)):
            @pl.when((source >= 0) & (source < line))
            def _(way=way, source=source):
                corner_wait(corner.at[side, source], ACROSS, corner_recv.at[source]).wait_recv()
                send_corner(way, source)
                send_corner(ACROSS, source)

    for way in (UP, DOWN, ACROSS):
        send_corner(way, at)

    def placed(value, shift):
        wide = value
        if total > 2 * own:
            zeros = jnp.zeros((value.shape[0], total - 2 * own), F32)
            wide = jnp.concatenate([value, zeros], axis=1)
        shift = shift * own % total
        return pltpu.roll(wide, shift, 1) if shift else wide

    inner = jnp.zeros((columns, total), F32)
    bands = []
    for index in range(rows):
        inner = inner + placed(pack[index, :columns, :], index - 1)
        block = placed(pack[index, columns : columns + own, :], index - 1)
        if index < rows - 1:
            block = block + placed(pack[index + 1, columns + own : columns + 2 * own, :], index + 1)
        bands.append(block)
    matrix = jnp.concatenate(bands, axis=0)
    orders = []
    for axis in range(2):
        value = lax.broadcasted_iota(jnp.int32, (total, total), axis)
        part, within = value // own, value % own
        sweep_own = spans * refl
        orders.append((within // sweep_own) * (rows * sweep_own) + part * sweep_own + within % sweep_own)
    down, over = orders
    earlier = (down // refl > over // refl) | ((down // refl == over // refl) & (down < over))
    matrix = jnp.where(earlier, matrix, jnp.where(down == over, 0.5 * matrix, 0.0))
    coeffs = precise_dot(inner, triangle_inverse(matrix, down, over, total), LAST)
    coeffs = pltpu.roll(coeffs, lax.rem(total + own - own * row, total), 1)[:, : 2 * own]
    coeffs = halves(coeffs)
    for step in range(2, line - 1):
        serve_all(0, step)

    @pl.loop(0, groups)
    def _(index):
        spread = spans_group(index)
        right = jnp.concatenate([jnp.zeros_like(spread), spread], axis=0)
        eig[:, cut_group(index)] -= dot_split(coeffs, halves(right), INNER)

    eig[:, :LANES] -= dot_split(coeffs, halves(jnp.concatenate([before, nothing], axis=0)), INNER)
    serve_all(0, line - 1)
    serve_corner(1)
    for panel in range(1, panels):
        send_own(ACROSS, panel)

    def reflectors(panel, where, parts):
        return jnp.concatenate([walls[panel][part[0], part[1], :, where] for part in parts], axis=0)

    def rounded(where):
        return eig[:, where].astype(BF16)

    def row_copy(source, dest, send, recv, step):
        bit = 2**step
        low_bit = (row // bit) % 2
        return pltpu.make_async_remote_copy(
            src_ref=source, dst_ref=dest, send_sem=send, recv_sem=recv,
            device_id={"row": row + bit * (1 - 2 * low_bit)}, device_id_type=pl.DeviceIdType.MESH,
        )

    steps = rows.bit_length() - 1
    kept = (columns + width, columns + early_width)

    def row_sum(panel, meanwhile):
        rows_at = pl.ds(0, kept[panel])
        for step in range(steps):
            move = row_copy(
                sums.at[panel, rows_at], got.at[panel, step, rows_at],
                sum_send.at[panel, step], sum_recv.at[panel, step], step,
            )
            move.start()
            if step == steps - 1:
                meanwhile()
            move.wait()
            sums[panel, rows_at, :] += got[panel, step, rows_at, :]

    def triangle(gram):
        down = lax.broadcasted_iota(jnp.int32, (width, width), 0)
        over = lax.broadcasted_iota(jnp.int32, (width, width), 1)
        matrix = jnp.where(down < over, gram, jnp.where(down == over, 0.5 * gram, 0.0))
        return triangle_inverse(matrix, down, over, width)

    def diagonal(parts):
        stack = []
        for part in parts:
            folded = corner[part[0], part[1]]
            stack.append(folded)
            for index in range(1, fold):
                stack.append(pltpu.roll(folded, LANES - index * width_own, 1))
        stack = jnp.concatenate(stack, axis=0)
        down = lax.broadcasted_iota(jnp.int32, (LANES, width), 0)
        over = lax.broadcasted_iota(jnp.int32, (LANES, width), 1) % width_own
        wide = precise_dot(stack, jnp.where(down == over, 1.0, 0.0).astype(F32))
        down = lax.broadcasted_iota(jnp.int32, (width, width), 0) // width_own
        over = lax.broadcasted_iota(jnp.int32, (width, width), 1) // width_own
        return jnp.where(down == over, wide, 0.0)

    def set_places(parts):
        for axis in range(2):
            part_at = lax.broadcasted_iota(jnp.int32, (width, width), axis) // width_own
            place = jnp.zeros_like(part_at)
            for index, part in enumerate(parts):
                place = jnp.where(part_at == index, 2 * part[1] + part[0], place)
            places[axis] = place

    def solved(gram, inner, inverse):
        down, over = places[0], places[1]
        if cols > 8:
            size = 1
            while size < cols:
                off = (down // (2 * size) == over // (2 * size)) & (down // size < over // size)
                off = halves(jnp.where(off, gram, 0.0))
                split = halves(inverse)
                inverse = inverse - dot_split(split, halves(dot_split(off, split, INNER)), INNER)
                size *= 2
            return dot_split(halves(inner), halves(inverse), LAST).astype(BF16)
        split = halves(inverse)
        power = halves(dot_split(split, halves(jnp.where(down < over, gram, 0.0)), INNER))
        value = dot_split(halves(inner), split, LAST)
        value = value - dot_split(halves(value), power, LAST)
        size = 2
        while size < cols:
            power = halves(dot_split(power, power, INNER))
            value = value + dot_split(halves(value), power, LAST)
            size *= 2
        return value.astype(BF16)

    for panel in range(panels):
        sums[panel] = jnp.zeros_like(sums[panel])
    late[...] = jnp.zeros_like(late)
    bulk[...] = jnp.zeros_like(bulk)
    for part in range(2):
        arrived(0, walls[0].at[other, :, :, span_of(part)], first_sem.at[part])

        @pl.loop(bounds[part], bounds[part + 1])
        def _(index):
            reflect = reflectors(0, cut(index), natural)
            left = jnp.concatenate([rounded(cut(index)), reflect], axis=0)
            sums[0] += lax.dot_general(left, reflect, LAST, preferred_element_type=F32)

        serve(1, 1, part)

    def serve_between():
        for step in range(2, line - 1):
            for part in range(2):
                serve(1, step, part)
        for part in range(2):
            serve_partner(part)

    serve_corner(2)
    row_sum(0, serve_between)
    for step in range(3, line):
        serve_corner(step)
    coeffs = precise_dot(sums[0, :columns, :], triangle(sums[0, columns:, :]), LAST).astype(BF16)

    @pl.loop(0, chunks)
    def _(index):
        reflect = reflectors(0, cut(index), natural)
        eig[:, cut(index)] -= lax.dot_general(coeffs, reflect, INNER, preferred_element_type=F32)

    early_parts, late_parts = order[:-2], order[-2:]

    for part in range(2):
        serve(1, line - 1, part)
        arrived(1, walls[1].at[other, pl.ds(0, line - 3), :, span_of(part)], early_sem.at[part])

        @pl.loop(bounds[part], bounds[part + 1])
        def _(index):
            reflect = reflectors(1, cut(index), early_parts)
            left = jnp.concatenate([rounded(cut(index)), reflect], axis=0)
            right = jnp.concatenate([reflect, jnp.zeros((late_width, chunk), BF16)], axis=0)
            sums[1, pl.ds(0, kept[1]), :] += lax.dot_general(left, right, LAST, preferred_element_type=F32)

    def add_late(where, sem, into):
        arrived(1, walls[1].at[other, pl.ds(0, 2), :, where], sem)
        reflect = reflectors(1, where, late_parts)
        right = jnp.concatenate([reflectors(1, where, order), rounded(where)], axis=0)
        into[...] += lax.dot_general(reflect, right, LAST, preferred_element_type=F32)

    def prepare():
        corner_wait(corner.at[other], ACROSS, corner_across).wait_recv()
        set_places(order)
        blocks[...] = diagonal(order)
        pl.loop(0, max(chunks - 2, 0))(lambda index: add_late(cut(index), last_sem.at[index], bulk))

    row_sum(1, prepare)
    def bulk_move(step):
        return row_copy(bulk, bulk_got.at[step], bulk_send.at[step], bulk_recv.at[step], step)

    bulk_move(0).start()
    for index in range(max(chunks - 2, 0), chunks - 1):
        add_late(cut(index), last_sem.at[index], late)
    for step in range(1, steps):
        bulk_move(step - 1).wait()
        bulk[...] += bulk_got[step - 1]
        bulk_move(step).start()
    for index, where in enumerate(closing):
        add_late(where, last_sem.at[chunks - 1 + index], late)

    def gone(ref, way, sem):
        pltpu.make_async_remote_copy(
            src_ref=ref, dst_ref=ref, send_sem=sem, recv_sem=partner_sem.at[0], device_id=target(way),
            device_id_type=pl.DeviceIdType.MESH,
        ).wait_send()

    def all_gone():
        for panel in range(panels):
            pieces = walls[panel].at[0]
            for place in range(line):
                @pl.when(at == place)
                def _(place=place):
                    above, below = place + 1, line - place
                    if panel == last:
                        above, below = above + 1 - place % 2, below + place % 2
                    if place < line - 1:
                        gone(pieces.at[pl.ds(0, above)], UP, send_sem.at[UP, panel])
                    if place > 0:
                        gone(pieces.at[pl.ds(0, below)], DOWN, send_sem.at[DOWN, panel])
            count = line - 1 if panel == last else line
            gone(pieces.at[pl.ds(0, count)], ACROSS, send_sem.at[ACROSS, panel])
        for place in range(line):
            @pl.when(at == place)
            def _(place=place):
                if place < line - 1:
                    corner_wait(corner.at[0, pl.ds(0, place + 1)], UP, corner_across).wait_send()
                if place > 0:
                    corner_wait(corner.at[0, pl.ds(0, line - place)], DOWN, corner_across).wait_send()
        corner_wait(corner.at[0], ACROSS, corner_across).wait_send()
        pl.when(row < rows - 1)(lambda: tail_copy().wait_send())
        pack_others().wait_send()

    for step in range(steps):
        if step == 0:
            move = row_copy(late, late_got, late_send.at[step], late_recv.at[step], step)
        else:
            late_cast[...] = late[...].astype(BF16)
            move = row_copy(late_cast, late_cast_got.at[step - 1], late_send.at[step], late_recv.at[step], step)
        move.start()
        if step == steps - 1:
            all_gone()
            bulk_move(step).wait()
            bulk[...] += bulk_got[step]
        move.wait()
        late[...] += late_got[...] if step == 0 else late_cast_got[step - 1].astype(F32)
    summed = late[...] + bulk[...]
    down = lax.broadcasted_iota(jnp.int32, (late_width, width), 0)
    over = lax.broadcasted_iota(jnp.int32, (late_width, width), 1)
    turn = jnp.where(down + early_width == over, 1.0, 0.0).astype(BF16)
    first_dim = (((0,), (0,)), ((), ()))
    turned = sum(lax.dot_general(part, turn, first_dim, preferred_element_type=F32) for part in halves(summed))
    gram = jnp.concatenate(
        [sums[1, columns : columns + early_width, :] + turned[:early_width], summed[:, :width]], axis=0
    )
    coef_ref[...] = solved(gram, sums[1, :columns, :] + turned[width:], blocks[...])


def finish_kernel(eig_ref, wall_ref, coef_ref, out_ref, held, sems):
    line = wall_ref.shape[1]
    rows_dev = eig_ref.shape[1]
    chunk = tile_of(rows_dev, 14)
    chunks = rows_dev // chunk

    def cut(index):
        return pl.ds(pl.multiple_of(index * chunk, chunk), chunk)

    def copy(index):
        return pltpu.make_async_copy(held.at[:, cut(index)], out_ref.at[:, cut(index)], sems.at[index])

    coeffs = coef_ref[...]
    col = lax.axis_index("col")
    order = last_order(line, col // 2, col % 2)

    for index in range(chunks):
        reflect = jnp.concatenate([wall_ref[part[0], part[1], :, cut(index)] for part in order], axis=0)
        update = lax.dot_general(coeffs, reflect, INNER, preferred_element_type=F32)
        held[:, cut(index)] = eig_ref[:, cut(index)] - update
        copy(index).start()

    @pl.loop(0, chunks)
    def _(index):
        copy(index).wait()


def local(eigvecs, span_vectors, span_offsets, panels):
    rows, cols = lax.axis_size("row"), lax.axis_size("col")
    columns, rows_dev = eigvecs.shape
    count, width_own, _ = panels.shape
    sweeps, spans, refl, band = span_vectors.shape
    own = sweeps * spans * refl
    width = width_own * cols
    steps = rows.bit_length() - 1
    chunks = rows_dev // tile_of(rows_dev, 14)
    late_width = 2 * width_own
    line = cols // 2
    vmem = pltpu.VMEM
    dma = pltpu.SemaphoreType.DMA
    eigen, wall, coeffs = pl.pallas_call(
        kernel,
        out_shape=(
            vmem(eigvecs.shape, F32),
            vmem((2, line, width_own, rows_dev), BF16),
            vmem((columns, width), BF16),
        ),
        in_specs=[pl.BlockSpec(memory_space=pltpu.HBM)] * 4,
        out_specs=[pl.BlockSpec(memory_space=pltpu.VMEM)] * 3,
        scratch_shapes=[
            vmem((2, line, width_own, rows_dev), BF16),
            vmem(span_vectors.shape, F32),
            pltpu.SMEM(span_offsets.shape, jnp.int32),
            vmem((own, LANES), F32),
            vmem((own, LANES), F32),
            vmem((own, LANES), jnp.int32),
            vmem((own, LANES), F32),
            vmem((own, LANES), F32),
            vmem((rows, columns + 2 * own + width_own, 2 * own), F32),
            vmem((count, columns + width, width), F32),
            vmem((count, steps, columns + width, width), F32),
            vmem((late_width, columns + width), F32),
            vmem((late_width, columns + width), F32),
            vmem((late_width, columns + width), BF16),
            vmem((steps, late_width, columns + width), BF16),
            vmem((late_width, columns + width), F32),
            vmem((steps, late_width, columns + width), F32),
            vmem((2, line, 8, LANES), F32),
            vmem((2, width, width), jnp.int32),
            vmem((width, width), F32),
            dma((3,)),
            dma((count,)),
            dma((count, line, 2)),
            dma((2,)),
            dma((2,)),
            dma((2,)),
            dma((chunks + 1,)),
            dma((3, count)),
            dma((2,)),
            dma,
            dma,
            dma((count, steps)),
            dma((count, steps)),
            dma((steps,)),
            dma((steps,)),
            dma((steps,)),
            dma((steps,)),
            dma((3,)),
            dma((line,)),
            dma,
        ],
        compiler_params=pltpu.CompilerParams(
            collective_id=0, has_side_effects=True, vmem_limit_bytes=40 * 2**20
        ),
        cost_estimate=pl.CostEstimate(
            flops=8 * width * (width + columns) * rows_dev,
            bytes_accessed=8 * rows_dev * columns + 8 * width * rows_dev,
            transcendentals=0,
        ),
    )(*(pltpu.with_memory_space_constraint(value, pltpu.HBM) for value in (eigvecs, span_vectors, span_offsets, panels)))
    return pl.pallas_call(
        finish_kernel,
        out_shape=jax.ShapeDtypeStruct(eigvecs.shape, F32),
        in_specs=[pl.BlockSpec(memory_space=pltpu.VMEM)] * 3,
        out_specs=pl.BlockSpec(memory_space=pl.ANY),
        scratch_shapes=[vmem(eigvecs.shape, F32), dma((rows_dev // tile_of(rows_dev, 14),))],
        compiler_params=pltpu.CompilerParams(vmem_limit_bytes=16 * 2**20),
        cost_estimate=pl.CostEstimate(
            flops=2 * width * columns * rows_dev, bytes_accessed=8 * columns * rows_dev, transcendentals=0
        ),
    )(eigen, wall, coeffs)


def solution(mesh):
    return jax.shard_map(
        local,
        mesh=mesh,
        in_specs=(
            P("col", "row"),
            P(None, "row", None, None),
            P(None, "row"),
            P(None, "col", "row"),
        ),
        out_specs=P("col", "row"),
        check_vma=False,
    )
```

```python
import functools

import jax
import jax.numpy as jnp
from jax import lax
from jax.experimental import pallas as pl
from jax.experimental.pallas import tpu as pltpu
from jax.sharding import PartitionSpec as P

PRECISE = lax.Precision.HIGHEST
LAST = (((1,), (1,)), ((), ()))
INNER = (((1,), (0,)), ((), ()))
LANES = 128
F32 = jnp.float32
BF16 = jnp.bfloat16
UP, DOWN, ACROSS = 0, 1, 2


def tile_of(rows_dev, most):
    count = rows_dev // LANES
    return LANES * max(part for part in range(1, most + 1) if count % part == 0)


def halves(value):
    high = value.astype(BF16)
    return high, (value - high.astype(F32)).astype(BF16)


def dot_split(left, right, dims):
    (left_high, left_low), (right_high, right_low) = left, right
    dot = functools.partial(lax.dot_general, dimension_numbers=dims, preferred_element_type=F32)
    return dot(left_high, right_high) + (dot(left_high, right_low) + dot(left_low, right_high))


def precise_dot(left, right, dims=INNER):
    return lax.dot_general(left, right, dims, precision=PRECISE, preferred_element_type=F32)


def triangle_inverse(matrix, down_at, across_at, order):
    same = down_at == across_at
    diagonal = jnp.where(same, matrix, 0.0)
    down = 1.0 / jnp.sum(diagonal, axis=1, keepdims=True)
    across = 1.0 / jnp.sum(diagonal, axis=0, keepdims=True)
    inverse = jnp.where(same, down, 0.0)
    beside = (down_at // 2 == across_at // 2) & (down_at != across_at)
    inverse = inverse - jnp.where(beside, matrix * down * across, 0.0)
    size = 2
    while size < order:
        together = down_at // (2 * size) == across_at // (2 * size)
        beside = together & (down_at // size != across_at // size)
        off = jnp.where(beside, matrix, 0.0)
        inverse = inverse - precise_dot(inverse, precise_dot(off, inverse))
        size *= 2
    return inverse


def natural_order(line):
    return [(side, place) for place in range(line) for side in range(2)]


def last_order(line, at, side):
    beside = at + 1 - 2 * (at % 2)
    far = (line - 1) * (1 - 2 * at // line)
    first, second = jnp.minimum(beside, far), jnp.maximum(beside, far)
    early = []
    for index in range(line - 2):
        place = index + jnp.where(first <= index, 1, 0)
        early.append(place + jnp.where(second <= place, 1, 0))
    order = [(side, place) for place in range(line)]
    return order + [(1 - side, place) for place in (*early, beside, far)]


def kernel(
    eig_ref, vec_ref, off_ref, pan_ref, eig, wall_last, coef_ref,
    wall_first, vecs, offs, low, high, base, tail_out, tail_in, pack, sums, got,
    late, late_got, late_cast, late_cast_got, bulk, bulk_got, corner, places, blocks,
    load_sem, own_sem, line_sem, first_sem, partner_sem, early_sem, last_sem, send_sem,
    tail_sem, pack_send, pack_recv, sum_send, sum_recv, late_send, late_recv,
    bulk_send, bulk_recv, corner_send, corner_recv, corner_across,
):
    rows, cols = lax.axis_size("row"), lax.axis_size("col")
    line = cols // 2
    row, col = lax.axis_index("row"), lax.axis_index("col")
    at, side = col // 2, col % 2
    columns, rows_dev = eig.shape
    walls = (wall_first, wall_last)
    panels, width_own, _ = pan_ref.shape
    width = cols * width_own
    sweeps, spans, refl, band = vecs.shape
    own = sweeps * spans * refl
    total = rows * own
    chunk = tile_of(rows_dev, 14)
    chunks = rows_dev // chunk
    tiles = rows_dev // LANES
    group = tile_of(rows_dev, 7)
    groups = rows_dev // group
    last = panels - 1
    beside = at + 1 - 2 * (at % 2)
    far = (line - 1) * (1 - 2 * at // line)
    other = 1 - side
    natural, order = natural_order(line), last_order(line, at, side)
    late_width = 2 * width_own
    early_width = width - late_width
    fold = width_own // 8
    bounds = (0, (chunks + 1) // 2, chunks)

    def cut(index):
        return pl.ds(pl.multiple_of(index * chunk, chunk), chunk)

    short = max(1, chunk // LANES // 4) * LANES
    closing = (
        pl.ds(rows_dev - chunk, chunk - short),
        pl.ds(rows_dev - short, short),
    )

    def span_of(part):
        return pl.ds(bounds[part] * chunk, (bounds[part + 1] - bounds[part]) * chunk)

    def target(way):
        if way == ACROSS:
            return {"col": col + 1 - 2 * side}
        return {"col": col + 2 if way == UP else col - 2}

    def guarded(way, start):
        if way == UP:
            pl.when(at < line - 1)(start)
        elif way == DOWN:
            pl.when(at > 0)(start)
        else:
            start()

    def copy(way, panel, piece, where, sem, mine=False):
        dest = walls[panel].at[piece[0], piece[1], :, where]
        return pltpu.make_async_remote_copy(
            src_ref=pan_ref.at[panel, :, where] if mine else dest,
            dst_ref=dest,
            send_sem=send_sem.at[way, panel],
            recv_sem=sem,
            device_id=target(way),
            device_id_type=pl.DeviceIdType.MESH,
        )

    def send(way, panel, piece, where, sem, mine=False):
        guarded(way, lambda: copy(way, panel, piece, where, sem, mine).start())

    def arrived(panel, ref, sem):
        pltpu.make_async_remote_copy(
            src_ref=ref, dst_ref=ref, send_sem=send_sem.at[ACROSS, panel], recv_sem=sem,
            device_id=target(ACROSS), device_id_type=pl.DeviceIdType.MESH,
        ).wait_recv()

    def send_own(way, panel):
        for part in range(2):
            if way == ACROSS:
                sem = partner_sem.at[part] if panel == last else first_sem.at[part]
            else:
                sem = line_sem.at[panel, at, part]
            send(way, panel, (side, at), span_of(part), sem, True)

    def send_last(way, piece, part):
        @pl.loop(bounds[part], min(bounds[part + 1], chunks - 1))
        def _(index):
            send(way, last, piece, cut(index), last_sem.at[index])

        if bounds[part + 1] == chunks:
            for index, where in enumerate(closing):
                send(way, last, piece, where, last_sem.at[chunks - 1 + index])

    def serve(panel, step, part):
        for way, source in ((UP, at - step), (DOWN, at + step)):
            @pl.when((source >= 0) & (source < line))
            def _(way=way, source=source):
                piece = (side, source)
                sem = line_sem.at[panel, source, part]
                arrived(panel, walls[panel].at[side, source, :, span_of(part)], sem)
                send(way, panel, piece, span_of(part), sem)
                if panel < last:
                    send(ACROSS, panel, piece, span_of(part), first_sem.at[part])
                    return

                @pl.when(source == far)
                def _():
                    send_last(ACROSS, piece, part)

                @pl.when((source != far) & (source != beside))
                def _():
                    send(ACROSS, panel, piece, span_of(part), early_sem.at[part])

    def serve_all(panel, step):
        for part in range(2):
            serve(panel, step, part)
        if panel < last:
            @pl.when(at == step)
            def _():
                send_own(UP, panel + 1)

            @pl.when(at == line - 1 - step)
            def _():
                send_own(DOWN, panel + 1)

    def serve_partner(part):
        arrived(last, walls[last].at[other, at, :, span_of(part)], partner_sem.at[part])
        for way in (UP, DOWN):
            @pl.when(at % 2 == way)
            def _(way=way):
                send_last(way, (other, at), part)

    vec_load = pltpu.make_async_copy(vec_ref, vecs, load_sem.at[1])
    off_load = pltpu.make_async_copy(off_ref, offs, load_sem.at[2])

    barrier = pltpu.get_barrier_semaphore()

    def greet(where):
        pl.semaphore_signal(barrier, inc=1, device_id=where, device_id_type=pl.DeviceIdType.MESH)

    greet(target(ACROSS))
    pl.when(at > 0)(lambda: greet(target(DOWN)))
    pl.when(at < line - 1)(lambda: greet(target(UP)))
    for step in range(1, rows):
        greet({"row": lax.rem(row + step, rows)})
    vec_load.start()
    off_load.start()
    neighbours = jnp.minimum(at, 1) + jnp.minimum(line - 1 - at, 1)
    pl.semaphore_wait(barrier, rows + neighbours)

    send_own(UP, 0)
    send_own(DOWN, 0)
    send_own(ACROSS, 0)
    load = pltpu.make_async_copy(eig_ref, eig, load_sem.at[0])
    load.start()
    for panel in range(panels):
        pltpu.make_async_copy(pan_ref.at[panel], walls[panel].at[side, at], own_sem.at[panel]).start()
    pl.when(at == 0)(lambda: send_own(UP, 1))
    pl.when(at == line - 1)(lambda: send_own(DOWN, 1))

    vec_load.wait()
    off_load.wait()

    for index in range(sweeps * spans):
        low[index * refl : (index + 1) * refl, :] = vecs[index // spans, index % spans]
    per = 8 // refl
    for index in range(own // 8):
        rows_at = slice(8 * index, 8 * index + 8)
        spread = jnp.concatenate([low[rows_at, :], jnp.zeros((8, LANES), F32)], axis=1)
        moved = jnp.zeros_like(spread)
        first = jnp.zeros((8, LANES), jnp.int32)
        for part in range(per):
            span_at = index * per + part
            begin = offs[span_at // spans, span_at % spans]
            tile = begin // LANES
            turned = pltpu.roll(spread, begin - tile * LANES, 1)
            place = lax.broadcasted_iota(jnp.int32, (8, 2 * LANES), 0) // refl
            moved = jnp.where(place == part, turned, moved)
            first = jnp.where(place[:, :LANES] == part, tile, first)
        low[rows_at, :] = moved[:, :LANES]
        high[rows_at, :] = moved[:, LANES:]
        base[rows_at, :] = first

    def spans_at(tile):
        part = jnp.where(base[...] == tile, low[...], 0.0)
        return part + jnp.where(base[...] == tile - 1, high[...], 0.0)

    def spans_group(index):
        first = index * (group // LANES)
        return jnp.concatenate([spans_at(first + step) for step in range(group // LANES)], axis=1)

    def cut_group(index):
        return pl.ds(pl.multiple_of(index * group, group), group)

    tail_out[...] = jnp.where(base[...] == tiles - 1, high[...], 0.0)

    def tail_copy():
        return pltpu.make_async_remote_copy(
            src_ref=tail_out, dst_ref=tail_in, send_sem=tail_sem.at[0], recv_sem=tail_sem.at[1],
            device_id={"row": row + 1}, device_id_type=pl.DeviceIdType.MESH,
        )

    pl.when(row < rows - 1)(lambda: tail_copy().start())
    for panel in range(panels):
        pltpu.make_async_copy(pan_ref.at[panel], walls[panel].at[side, at], own_sem.at[panel]).wait()

    def own_products(index, acc):
        mine = walls[last][side, at, :, cut(index)]
        padded = jnp.concatenate([mine, jnp.zeros((LANES - width_own, chunk), BF16)], axis=0)
        return acc + lax.dot_general(mine, padded, LAST, preferred_element_type=F32)

    pack[row, columns + 2 * own :, :] = lax.fori_loop(0, chunks, own_products, jnp.zeros((width_own, LANES), F32))
    load.wait()

    def products(index, acc):
        spread = spans_group(index)
        left = jnp.concatenate([eig[:, cut_group(index)], spread], axis=0)
        right = jnp.concatenate([jnp.zeros_like(spread), spread], axis=0)
        return acc + dot_split(halves(left), halves(right), LAST)

    acc = lax.fori_loop(0, groups, products, jnp.zeros((columns + own, 2 * own), F32))
    pl.when(row > 0)(lambda: tail_copy().wait_recv())

    @pl.when(row == 0)
    def _():
        tail_in[...] = jnp.zeros_like(tail_in)

    before = tail_in[...]
    head = spans_at(0)
    nothing = jnp.zeros_like(before)
    left = jnp.concatenate([eig[:, :LANES], head], axis=0)
    acc = acc + dot_split(halves(left), halves(jnp.concatenate([before, nothing], axis=0)), LAST)
    tail = tail_out[...]
    beyond = dot_split(halves(tail), halves(jnp.concatenate([nothing, tail], axis=0)), LAST)
    pack[row, :columns, :] = acc[:columns]
    pack[row, columns : columns + own, :] = acc[columns:] + beyond
    pack[row, columns + own : columns + 2 * own, :] = dot_split(
        halves(before), halves(jnp.concatenate([head, nothing], axis=0)), LAST
    )

    def pack_copy(step):
        return pltpu.make_async_remote_copy(
            src_ref=pack.at[row], dst_ref=pack.at[row], send_sem=pack_send, recv_sem=pack_recv,
            device_id={"row": lax.rem(row + step, rows)}, device_id_type=pl.DeviceIdType.MESH,
        )

    def pack_others():
        ref = pack.at[pl.ds(0, rows - 1)]
        return pltpu.make_async_remote_copy(
            src_ref=ref, dst_ref=ref, send_sem=pack_send, recv_sem=pack_recv,
            device_id={"row": lax.rem(row + 1, rows)}, device_id_type=pl.DeviceIdType.MESH,
        )

    for step in range(1, rows):
        pack_copy(step).start()
    serve_all(0, 1)
    pack_others().wait_recv()

    square = pack[0, columns + 2 * own :, :]
    for index in range(1, rows):
        square = square + pack[index, columns + 2 * own :, :]
    square = square[:, :width_own]
    down = lax.broadcasted_iota(jnp.int32, (width_own, width_own), 0)
    over = lax.broadcasted_iota(jnp.int32, (width_own, width_own), 1)
    square = jnp.where(down < over, square, jnp.where(down == over, 0.5 * square, 0.0))
    square = triangle_inverse(square, down, over, width_own)
    square = jnp.concatenate([square, jnp.zeros((width_own, LANES - width_own), F32)], axis=1)
    folded = square[:8]
    for index in range(1, fold):
        folded = folded + pltpu.roll(square[8 * index : 8 * index + 8], index * width_own, 1)
    corner[side, at] = folded

    def send_corner(way, source):
        ref = corner.at[side, source]
        move = pltpu.make_async_remote_copy(
            src_ref=ref, dst_ref=ref, send_sem=corner_send.at[way],
            recv_sem=corner_across if way == ACROSS else corner_recv.at[source],
            device_id=target(way), device_id_type=pl.DeviceIdType.MESH,
        )
        guarded(way, move.start)

    def corner_wait(ref, way, sem):
        return pltpu.make_async_remote_copy(
            src_ref=ref, dst_ref=ref, send_sem=corner_send.at[way], recv_sem=sem,
            device_id=target(way), device_id_type=pl.DeviceIdType.MESH,
        )

    def serve_corner(step):
        for way, source in ((UP, at - step), (DOWN, at + step)):
            @pl.when((source >= 0) & (source < line))
            def _(way=way, source=source):
                corner_wait(corner.at[side, source], ACROSS, corner_recv.at[source]).wait_recv()
                send_corner(way, source)
                send_corner(ACROSS, source)

    for way in (UP, DOWN, ACROSS):
        send_corner(way, at)

    def placed(value, shift):
        wide = value
        if total > 2 * own:
            zeros = jnp.zeros((value.shape[0], total - 2 * own), F32)
            wide = jnp.concatenate([value, zeros], axis=1)
        shift = shift * own % total
        return pltpu.roll(wide, shift, 1) if shift else wide

    inner = jnp.zeros((columns, total), F32)
    bands = []
    for index in range(rows):
        inner = inner + placed(pack[index, :columns, :], index - 1)
        block = placed(pack[index, columns : columns + own, :], index - 1)
        if index < rows - 1:
            block = block + placed(pack[index + 1, columns + own : columns + 2 * own, :], index + 1)
        bands.append(block)
    matrix = jnp.concatenate(bands, axis=0)
    orders = []
    for axis in range(2):
        value = lax.broadcasted_iota(jnp.int32, (total, total), axis)
        part, within = value // own, value % own
        sweep_own = spans * refl
        orders.append((within // sweep_own) * (rows * sweep_own) + part * sweep_own + within % sweep_own)
    down, over = orders
    earlier = (down // refl > over // refl) | ((down // refl == over // refl) & (down < over))
    matrix = jnp.where(earlier, matrix, jnp.where(down == over, 0.5 * matrix, 0.0))
    coeffs = precise_dot(inner, triangle_inverse(matrix, down, over, total), LAST)
    coeffs = pltpu.roll(coeffs, lax.rem(total + own - own * row, total), 1)[:, : 2 * own]
    coeffs = halves(coeffs)
    for step in range(2, line - 1):
        serve_all(0, step)

    @pl.loop(0, groups)
    def _(index):
        spread = spans_group(index)
        right = jnp.concatenate([jnp.zeros_like(spread), spread], axis=0)
        eig[:, cut_group(index)] -= dot_split(coeffs, halves(right), INNER)

    eig[:, :LANES] -= dot_split(coeffs, halves(jnp.concatenate([before, nothing], axis=0)), INNER)
    serve_all(0, line - 1)
    serve_corner(1)
    for panel in range(1, panels):
        send_own(ACROSS, panel)

    def reflectors(panel, where, parts):
        return jnp.concatenate([walls[panel][part[0], part[1], :, where] for part in parts], axis=0)

    def rounded(where):
        return eig[:, where].astype(BF16)

    def row_copy(source, dest, send, recv, step):
        bit = 2**step
        low_bit = (row // bit) % 2
        return pltpu.make_async_remote_copy(
            src_ref=source, dst_ref=dest, send_sem=send, recv_sem=recv,
            device_id={"row": row + bit * (1 - 2 * low_bit)}, device_id_type=pl.DeviceIdType.MESH,
        )

    steps = rows.bit_length() - 1
    kept = (columns + width, columns + early_width)

    def row_sum(panel, meanwhile):
        rows_at = pl.ds(0, kept[panel])
        for step in range(steps):
            move = row_copy(
                sums.at[panel, rows_at], got.at[panel, step, rows_at],
                sum_send, sum_recv.at[panel, step], step,
            )
            move.start()
            if step == steps - 1:
                meanwhile()
            move.wait()
            sums[panel, rows_at, :] += got[panel, step, rows_at, :]

    def triangle(gram):
        down = lax.broadcasted_iota(jnp.int32, (width, width), 0)
        over = lax.broadcasted_iota(jnp.int32, (width, width), 1)
        matrix = jnp.where(down < over, gram, jnp.where(down == over, 0.5 * gram, 0.0))
        return triangle_inverse(matrix, down, over, width)

    def diagonal(parts):
        stack = []
        for part in parts:
            folded = corner[part[0], part[1]]
            stack.append(folded)
            for index in range(1, fold):
                stack.append(pltpu.roll(folded, LANES - index * width_own, 1))
        stack = jnp.concatenate(stack, axis=0)
        down = lax.broadcasted_iota(jnp.int32, (LANES, width), 0)
        over = lax.broadcasted_iota(jnp.int32, (LANES, width), 1) % width_own
        wide = precise_dot(stack, jnp.where(down == over, 1.0, 0.0).astype(F32))
        down = lax.broadcasted_iota(jnp.int32, (width, width), 0) // width_own
        over = lax.broadcasted_iota(jnp.int32, (width, width), 1) // width_own
        return jnp.where(down == over, wide, 0.0)

    def set_places(parts):
        for axis in range(2):
            part_at = lax.broadcasted_iota(jnp.int32, (width, width), axis) // width_own
            place = jnp.zeros_like(part_at)
            for index, part in enumerate(parts):
                place = jnp.where(part_at == index, 2 * part[1] + part[0], place)
            places[axis] = place

    def solved(gram, inner, inverse):
        down, over = places[0], places[1]
        if cols > 8:
            size = 1
            while size < cols:
                off = (down // (2 * size) == over // (2 * size)) & (down // size < over // size)
                off = halves(jnp.where(off, gram, 0.0))
                split = halves(inverse)
                inverse = inverse - dot_split(split, halves(dot_split(off, split, INNER)), INNER)
                size *= 2
            return dot_split(halves(inner), halves(inverse), LAST).astype(BF16)
        split = halves(inverse)
        power = halves(dot_split(split, halves(jnp.where(down < over, gram, 0.0)), INNER))
        value = dot_split(halves(inner), split, LAST)
        value = value - dot_split(halves(value), power, LAST)
        size = 2
        while size < cols:
            power = halves(dot_split(power, power, INNER))
            value = value + dot_split(halves(value), power, LAST)
            size *= 2
        return value.astype(BF16)

    for panel in range(panels):
        sums[panel] = jnp.zeros_like(sums[panel])
    late[...] = jnp.zeros_like(late)
    bulk[...] = jnp.zeros_like(bulk)
    for part in range(2):
        arrived(0, walls[0].at[other, :, :, span_of(part)], first_sem.at[part])

        @pl.loop(bounds[part], bounds[part + 1])
        def _(index):
            reflect = reflectors(0, cut(index), natural)
            left = jnp.concatenate([rounded(cut(index)), reflect], axis=0)
            sums[0] += lax.dot_general(left, reflect, LAST, preferred_element_type=F32)

        serve(1, 1, part)

    def serve_between():
        for step in range(2, line - 1):
            for part in range(2):
                serve(1, step, part)
        for part in range(2):
            serve_partner(part)

    serve_corner(2)
    row_sum(0, serve_between)
    for step in range(3, line):
        serve_corner(step)
    coeffs = precise_dot(sums[0, :columns, :], triangle(sums[0, columns:, :]), LAST).astype(BF16)

    @pl.loop(0, chunks)
    def _(index):
        reflect = reflectors(0, cut(index), natural)
        eig[:, cut(index)] -= lax.dot_general(coeffs, reflect, INNER, preferred_element_type=F32)

    early_parts, late_parts = order[:-2], order[-2:]

    for part in range(2):
        serve(1, line - 1, part)
        arrived(1, walls[1].at[other, pl.ds(0, line - 3), :, span_of(part)], early_sem.at[part])

        @pl.loop(bounds[part], bounds[part + 1])
        def _(index):
            reflect = reflectors(1, cut(index), early_parts)
            left = jnp.concatenate([rounded(cut(index)), reflect], axis=0)
            right = jnp.concatenate([reflect, jnp.zeros((late_width, chunk), BF16)], axis=0)
            sums[1, pl.ds(0, kept[1]), :] += lax.dot_general(left, right, LAST, preferred_element_type=F32)

    def add_late(where, sem, into):
        arrived(1, walls[1].at[other, pl.ds(0, 2), :, where], sem)
        reflect = reflectors(1, where, late_parts)
        right = jnp.concatenate([reflectors(1, where, order), rounded(where)], axis=0)
        into[...] += lax.dot_general(reflect, right, LAST, preferred_element_type=F32)

    def prepare():
        corner_wait(corner.at[other], ACROSS, corner_across).wait_recv()
        set_places(order)
        blocks[...] = diagonal(order)
        pl.loop(0, max(chunks - 2, 0))(lambda index: add_late(cut(index), last_sem.at[index], bulk))

    row_sum(1, prepare)
    def bulk_move(step):
        return row_copy(bulk, bulk_got.at[step], bulk_send, bulk_recv.at[step], step)

    bulk_move(0).start()
    for index in range(max(chunks - 2, 0), chunks - 1):
        add_late(cut(index), last_sem.at[index], late)
    for step in range(1, steps):
        bulk_move(step - 1).wait()
        bulk[...] += bulk_got[step - 1]
        bulk_move(step).start()
    for index, where in enumerate(closing):
        add_late(where, last_sem.at[chunks - 1 + index], late)

    def gone(ref, way, sem):
        pltpu.make_async_remote_copy(
            src_ref=ref, dst_ref=ref, send_sem=sem, recv_sem=partner_sem.at[0], device_id=target(way),
            device_id_type=pl.DeviceIdType.MESH,
        ).wait_send()

    def all_gone():
        for panel in range(panels):
            pieces = walls[panel].at[0]
            for place in range(line):
                @pl.when(at == place)
                def _(place=place):
                    above, below = place + 1, line - place
                    if panel == last:
                        above, below = above + 1 - place % 2, below + place % 2
                    if place < line - 1:
                        gone(pieces.at[pl.ds(0, above)], UP, send_sem.at[UP, panel])
                    if place > 0:
                        gone(pieces.at[pl.ds(0, below)], DOWN, send_sem.at[DOWN, panel])
            count = line - 1 if panel == last else line
            gone(pieces.at[pl.ds(0, count)], ACROSS, send_sem.at[ACROSS, panel])
        for place in range(line):
            @pl.when(at == place)
            def _(place=place):
                if place < line - 1:
                    corner_wait(corner.at[0, pl.ds(0, place + 1)], UP, corner_across).wait_send()
                if place > 0:
                    corner_wait(corner.at[0, pl.ds(0, line - place)], DOWN, corner_across).wait_send()
        corner_wait(corner.at[0], ACROSS, corner_across).wait_send()
        pl.when(row < rows - 1)(lambda: tail_copy().wait_send())
        pack_others().wait_send()

    for step in range(steps):
        if step == 0:
            move = row_copy(late, late_got, late_send, late_recv.at[step], step)
        else:
            late_cast[...] = late[...].astype(BF16)
            move = row_copy(late_cast, late_cast_got.at[step - 1], late_send, late_recv.at[step], step)
        move.start()
        if step == steps - 1:
            all_gone()
            bulk_move(step).wait()
            bulk[...] += bulk_got[step]
        move.wait()
        late[...] += late_got[...] if step == 0 else late_cast_got[step - 1].astype(F32)
    summed = late[...] + bulk[...]
    down = lax.broadcasted_iota(jnp.int32, (late_width, width), 0)
    over = lax.broadcasted_iota(jnp.int32, (late_width, width), 1)
    turn = jnp.where(down + early_width == over, 1.0, 0.0).astype(BF16)
    first_dim = (((0,), (0,)), ((), ()))
    turned = sum(lax.dot_general(part, turn, first_dim, preferred_element_type=F32) for part in halves(summed))
    gram = jnp.concatenate(
        [sums[1, columns : columns + early_width, :] + turned[:early_width], summed[:, :width]], axis=0
    )
    coef_ref[...] = solved(gram, sums[1, :columns, :] + turned[width:], blocks[...])


def finish_kernel(eig_ref, wall_ref, coef_ref, out_ref, held, sems):
    line = wall_ref.shape[1]
    rows_dev = eig_ref.shape[1]
    chunk = tile_of(rows_dev, 14)
    pieces, begin = [], 0
    while begin < rows_dev:
        size = min(chunk // 2 // LANES * LANES if not pieces else chunk, rows_dev - begin)
        pieces.append(pl.ds(begin, size))
        begin += size

    def copy(index):
        where = pieces[index]
        return pltpu.make_async_copy(held.at[:, where], out_ref.at[:, where], sems.at[index])

    coeffs = coef_ref[...]
    col = lax.axis_index("col")
    order = last_order(line, col // 2, col % 2)
    for index, where in enumerate(pieces):
        reflect = jnp.concatenate([wall_ref[part[0], part[1], :, where] for part in order], axis=0)
        update = lax.dot_general(coeffs, reflect, INNER, preferred_element_type=F32)
        held[:, where] = eig_ref[:, where] - update
        copy(index).start()
    for index in range(len(pieces)):
        copy(index).wait()


def local(eigvecs, span_vectors, span_offsets, panels):
    rows, cols = lax.axis_size("row"), lax.axis_size("col")
    columns, rows_dev = eigvecs.shape
    count, width_own, _ = panels.shape
    sweeps, spans, refl, band = span_vectors.shape
    own = sweeps * spans * refl
    width = width_own * cols
    steps = rows.bit_length() - 1
    chunks = rows_dev // tile_of(rows_dev, 14)
    late_width = 2 * width_own
    line = cols // 2
    vmem = pltpu.VMEM
    dma = pltpu.SemaphoreType.DMA
    eigen, wall, coeffs = pl.pallas_call(
        kernel,
        out_shape=(
            vmem(eigvecs.shape, F32),
            vmem((2, line, width_own, rows_dev), BF16),
            vmem((columns, width), BF16),
        ),
        in_specs=[pl.BlockSpec(memory_space=pltpu.HBM)] * 4,
        out_specs=[pl.BlockSpec(memory_space=pltpu.VMEM)] * 3,
        scratch_shapes=[
            vmem((2, line, width_own, rows_dev), BF16),
            vmem(span_vectors.shape, F32),
            pltpu.SMEM(span_offsets.shape, jnp.int32),
            vmem((own, LANES), F32),
            vmem((own, LANES), F32),
            vmem((own, LANES), jnp.int32),
            vmem((own, LANES), F32),
            vmem((own, LANES), F32),
            vmem((rows, columns + 2 * own + width_own, 2 * own), F32),
            vmem((count, columns + width, width), F32),
            vmem((count, steps, columns + width, width), F32),
            vmem((late_width, columns + width), F32),
            vmem((late_width, columns + width), F32),
            vmem((late_width, columns + width), BF16),
            vmem((steps, late_width, columns + width), BF16),
            vmem((late_width, columns + width), F32),
            vmem((steps, late_width, columns + width), F32),
            vmem((2, line, 8, LANES), F32),
            vmem((2, width, width), jnp.int32),
            vmem((width, width), F32),
            dma((3,)),
            dma((count,)),
            dma((count, line, 2)),
            dma((2,)),
            dma((2,)),
            dma((2,)),
            dma((chunks + 1,)),
            dma((3, count)),
            dma((2,)),
            dma,
            dma,
            dma,
            dma((count, steps)),
            dma,
            dma((steps,)),
            dma,
            dma((steps,)),
            dma((3,)),
            dma((line,)),
            dma,
        ],
        compiler_params=pltpu.CompilerParams(
            collective_id=0, has_side_effects=True, vmem_limit_bytes=40 * 2**20
        ),
        cost_estimate=pl.CostEstimate(
            flops=8 * width * (width + columns) * rows_dev,
            bytes_accessed=8 * rows_dev * columns + 8 * width * rows_dev,
            transcendentals=0,
        ),
    )(*(pltpu.with_memory_space_constraint(value, pltpu.HBM) for value in (eigvecs, span_vectors, span_offsets, panels)))
    return pl.pallas_call(
        finish_kernel,
        out_shape=jax.ShapeDtypeStruct(eigvecs.shape, F32),
        in_specs=[pl.BlockSpec(memory_space=pltpu.VMEM)] * 3,
        out_specs=pl.BlockSpec(memory_space=pl.ANY),
        scratch_shapes=[vmem(eigvecs.shape, F32), dma((rows_dev // tile_of(rows_dev, 14) + 1,))],
        compiler_params=pltpu.CompilerParams(vmem_limit_bytes=16 * 2**20),
        cost_estimate=pl.CostEstimate(
            flops=2 * width * columns * rows_dev, bytes_accessed=8 * columns * rows_dev, transcendentals=0
        ),
    )(eigen, wall, coeffs)


def solution(mesh):
    return jax.shard_map(
        local,
        mesh=mesh,
        in_specs=(
            P("col", "row"),
            P(None, "row", None, None),
            P(None, "row"),
            P(None, "col", "row"),
        ),
        out_specs=P("col", "row"),
        check_vma=False,
    )
```

```python
import functools

import jax
import jax.numpy as jnp
from jax import lax
from jax.experimental import pallas as pl
from jax.experimental.pallas import tpu as pltpu
from jax.sharding import PartitionSpec as P

PRECISE = lax.Precision.HIGHEST
LAST = (((1,), (1,)), ((), ()))
INNER = (((1,), (0,)), ((), ()))
LANES = 128
F32 = jnp.float32
BF16 = jnp.bfloat16
UP, DOWN, ACROSS = 0, 1, 2


def tile_of(rows_dev, most):
    count = rows_dev // LANES
    return LANES * max(part for part in range(1, most + 1) if count % part == 0)


def halves(value):
    high = value.astype(BF16)
    return high, (value - high.astype(F32)).astype(BF16)


def dot_split(left, right, dims):
    (left_high, left_low), (right_high, right_low) = left, right
    dot = functools.partial(lax.dot_general, dimension_numbers=dims, preferred_element_type=F32)
    return dot(left_high, right_high) + (dot(left_high, right_low) + dot(left_low, right_high))


def precise_dot(left, right, dims=INNER):
    return lax.dot_general(left, right, dims, precision=PRECISE, preferred_element_type=F32)


def triangle_inverse(matrix, down_at, across_at, order):
    same = down_at == across_at
    diagonal = jnp.where(same, matrix, 0.0)
    down = 1.0 / jnp.sum(diagonal, axis=1, keepdims=True)
    across = 1.0 / jnp.sum(diagonal, axis=0, keepdims=True)
    inverse = jnp.where(same, down, 0.0)
    beside = (down_at // 2 == across_at // 2) & (down_at != across_at)
    inverse = inverse - jnp.where(beside, matrix * down * across, 0.0)
    size = 2
    while size < order:
        together = down_at // (2 * size) == across_at // (2 * size)
        beside = together & (down_at // size != across_at // size)
        off = jnp.where(beside, matrix, 0.0)
        inverse = inverse - precise_dot(inverse, precise_dot(off, inverse))
        size *= 2
    return inverse


def natural_order(line):
    return [(side, place) for place in range(line) for side in range(2)]


def last_order(line, at, side):
    beside = at + 1 - 2 * (at % 2)
    far = (line - 1) * (1 - 2 * at // line)
    first, second = jnp.minimum(beside, far), jnp.maximum(beside, far)
    early = []
    for index in range(line - 2):
        place = index + jnp.where(first <= index, 1, 0)
        early.append(place + jnp.where(second <= place, 1, 0))
    order = [(side, place) for place in range(line)]
    return order + [(1 - side, place) for place in (*early, beside, far)]


def kernel(
    eig_ref, vec_ref, off_ref, pan_ref, eig, wall_last, coef_ref,
    wall_first, vecs, offs, low, high, base, tail_out, tail_in, pack, sums, got,
    late, late_got, late_cast, late_cast_got, bulk, bulk_got, corner, places, blocks,
    load_sem, own_sem, line_sem, first_sem, partner_sem, early_sem, last_sem, send_sem,
    tail_sem, pack_send, pack_recv, sum_send, sum_recv, late_send, late_recv,
    bulk_send, bulk_recv, corner_send, corner_recv, corner_across,
):
    rows, cols = lax.axis_size("row"), lax.axis_size("col")
    line = cols // 2
    row, col = lax.axis_index("row"), lax.axis_index("col")
    at, side = col // 2, col % 2
    columns, rows_dev = eig.shape
    walls = (wall_first, wall_last)
    panels, width_own, _ = pan_ref.shape
    width = cols * width_own
    sweeps, spans, refl, band = vecs.shape
    own = sweeps * spans * refl
    total = rows * own
    chunk = tile_of(rows_dev, 14)
    chunks = rows_dev // chunk
    tiles = rows_dev // LANES
    group = tile_of(rows_dev, 7)
    groups = rows_dev // group
    last = panels - 1
    beside = at + 1 - 2 * (at % 2)
    far = (line - 1) * (1 - 2 * at // line)
    other = 1 - side
    natural, order = natural_order(line), last_order(line, at, side)
    late_width = 2 * width_own
    early_width = width - late_width
    fold = width_own // 8
    bounds = (0, (chunks + 1) // 2, chunks)

    def cut(index):
        return pl.ds(pl.multiple_of(index * chunk, chunk), chunk)

    short = max(1, chunk // LANES // 2) * LANES
    closing = (
        pl.ds(rows_dev - chunk, chunk - short),
        pl.ds(rows_dev - short, short),
    )

    def span_of(part):
        return pl.ds(bounds[part] * chunk, (bounds[part + 1] - bounds[part]) * chunk)

    def target(way):
        if way == ACROSS:
            return {"col": col + 1 - 2 * side}
        return {"col": col + 2 if way == UP else col - 2}

    def guarded(way, start):
        if way == UP:
            pl.when(at < line - 1)(start)
        elif way == DOWN:
            pl.when(at > 0)(start)
        else:
            start()

    def copy(way, panel, piece, where, sem, mine=False):
        dest = walls[panel].at[piece[0], piece[1], :, where]
        return pltpu.make_async_remote_copy(
            src_ref=pan_ref.at[panel, :, where] if mine else dest,
            dst_ref=dest,
            send_sem=send_sem.at[way, panel],
            recv_sem=sem,
            device_id=target(way),
            device_id_type=pl.DeviceIdType.MESH,
        )

    def send(way, panel, piece, where, sem, mine=False):
        guarded(way, lambda: copy(way, panel, piece, where, sem, mine).start())

    def arrived(panel, ref, sem):
        pltpu.make_async_remote_copy(
            src_ref=ref, dst_ref=ref, send_sem=send_sem.at[ACROSS, panel], recv_sem=sem,
            device_id=target(ACROSS), device_id_type=pl.DeviceIdType.MESH,
        ).wait_recv()

    def send_own(way, panel):
        for part in range(2):
            if way == ACROSS:
                sem = partner_sem.at[part] if panel == last else first_sem.at[part]
            else:
                sem = line_sem.at[panel, at, part]
            send(way, panel, (side, at), span_of(part), sem, True)

    def send_last(way, piece, part):
        @pl.loop(bounds[part], min(bounds[part + 1], chunks - 1))
        def _(index):
            send(way, last, piece, cut(index), last_sem.at[index])

        if bounds[part + 1] == chunks:
            for index, where in enumerate(closing):
                send(way, last, piece, where, last_sem.at[chunks - 1 + index])

    def serve(panel, step, part):
        for way, source in ((UP, at - step), (DOWN, at + step)):
            @pl.when((source >= 0) & (source < line))
            def _(way=way, source=source):
                piece = (side, source)
                sem = line_sem.at[panel, source, part]
                arrived(panel, walls[panel].at[side, source, :, span_of(part)], sem)
                send(way, panel, piece, span_of(part), sem)
                if panel < last:
                    send(ACROSS, panel, piece, span_of(part), first_sem.at[part])
                    return

                @pl.when(source == far)
                def _():
                    send_last(ACROSS, piece, part)

                @pl.when((source != far) & (source != beside))
                def _():
                    send(ACROSS, panel, piece, span_of(part), early_sem.at[part])

    def serve_all(panel, step):
        for part in range(2):
            serve(panel, step, part)
        if panel < last:
            @pl.when(at == step)
            def _():
                send_own(UP, panel + 1)

            @pl.when(at == line - 1 - step)
            def _():
                send_own(DOWN, panel + 1)

    def serve_partner(part):
        arrived(last, walls[last].at[other, at, :, span_of(part)], partner_sem.at[part])
        for way in (UP, DOWN):
            @pl.when(at % 2 == way)
            def _(way=way):
                send_last(way, (other, at), part)

    vec_load = pltpu.make_async_copy(vec_ref, vecs, load_sem.at[1])
    off_load = pltpu.make_async_copy(off_ref, offs, load_sem.at[2])
    vec_load.start()
    off_load.start()

    barrier = pltpu.get_barrier_semaphore()

    def greet(where):
        pl.semaphore_signal(barrier, inc=1, device_id=where, device_id_type=pl.DeviceIdType.MESH)

    greet(target(ACROSS))
    pl.when(at > 0)(lambda: greet(target(DOWN)))
    pl.when(at < line - 1)(lambda: greet(target(UP)))
    for step in range(1, rows):
        greet({"row": lax.rem(row + step, rows)})
    neighbours = jnp.minimum(at, 1) + jnp.minimum(line - 1 - at, 1)
    pl.semaphore_wait(barrier, rows + neighbours)

    send_own(UP, 0)
    send_own(DOWN, 0)
    send_own(ACROSS, 0)
    load = pltpu.make_async_copy(eig_ref, eig, load_sem.at[0])
    load.start()
    for panel in range(panels):
        pltpu.make_async_copy(pan_ref.at[panel], walls[panel].at[side, at], own_sem.at[panel]).start()
    pl.when(at == 0)(lambda: send_own(UP, 1))
    pl.when(at == line - 1)(lambda: send_own(DOWN, 1))

    vec_load.wait()
    off_load.wait()

    for index in range(sweeps * spans):
        low[index * refl : (index + 1) * refl, :] = vecs[index // spans, index % spans]
    per = 8 // refl
    for index in range(own // 8):
        rows_at = slice(8 * index, 8 * index + 8)
        spread = jnp.concatenate([low[rows_at, :], jnp.zeros((8, LANES), F32)], axis=1)
        moved = jnp.zeros_like(spread)
        first = jnp.zeros((8, LANES), jnp.int32)
        for part in range(per):
            span_at = index * per + part
            begin = offs[span_at // spans, span_at % spans]
            tile = begin // LANES
            turned = pltpu.roll(spread, begin - tile * LANES, 1)
            place = lax.broadcasted_iota(jnp.int32, (8, 2 * LANES), 0) // refl
            moved = jnp.where(place == part, turned, moved)
            first = jnp.where(place[:, :LANES] == part, tile, first)
        low[rows_at, :] = moved[:, :LANES]
        high[rows_at, :] = moved[:, LANES:]
        base[rows_at, :] = first

    def spans_at(tile):
        part = jnp.where(base[...] == tile, low[...], 0.0)
        return part + jnp.where(base[...] == tile - 1, high[...], 0.0)

    def spans_group(index):
        first = index * (group // LANES)
        return jnp.concatenate([spans_at(first + step) for step in range(group // LANES)], axis=1)

    def cut_group(index):
        return pl.ds(pl.multiple_of(index * group, group), group)

    tail_out[...] = jnp.where(base[...] == tiles - 1, high[...], 0.0)

    def tail_copy():
        return pltpu.make_async_remote_copy(
            src_ref=tail_out, dst_ref=tail_in, send_sem=tail_sem.at[0], recv_sem=tail_sem.at[1],
            device_id={"row": row + 1}, device_id_type=pl.DeviceIdType.MESH,
        )

    pl.when(row < rows - 1)(lambda: tail_copy().start())
    for panel in range(panels):
        pltpu.make_async_copy(pan_ref.at[panel], walls[panel].at[side, at], own_sem.at[panel]).wait()

    def own_products(index, acc):
        mine = walls[last][side, at, :, cut(index)]
        padded = jnp.concatenate([mine, jnp.zeros((LANES - width_own, chunk), BF16)], axis=0)
        return acc + lax.dot_general(mine, padded, LAST, preferred_element_type=F32)

    pack[row, columns + 2 * own :, :] = lax.fori_loop(0, chunks, own_products, jnp.zeros((width_own, LANES), F32))
    load.wait()

    def products(index, acc):
        spread = spans_group(index)
        left = jnp.concatenate([eig[:, cut_group(index)], spread], axis=0)
        right = jnp.concatenate([jnp.zeros_like(spread), spread], axis=0)
        return acc + dot_split(halves(left), halves(right), LAST)

    acc = lax.fori_loop(0, groups, products, jnp.zeros((columns + own, 2 * own), F32))
    pl.when(row > 0)(lambda: tail_copy().wait_recv())

    @pl.when(row == 0)
    def _():
        tail_in[...] = jnp.zeros_like(tail_in)

    before = tail_in[...]
    head = spans_at(0)
    nothing = jnp.zeros_like(before)
    left = jnp.concatenate([eig[:, :LANES], head], axis=0)
    acc = acc + dot_split(halves(left), halves(jnp.concatenate([before, nothing], axis=0)), LAST)
    tail = tail_out[...]
    beyond = dot_split(halves(tail), halves(jnp.concatenate([nothing, tail], axis=0)), LAST)
    pack[row, :columns, :] = acc[:columns]
    pack[row, columns : columns + own, :] = acc[columns:] + beyond
    pack[row, columns + own : columns + 2 * own, :] = dot_split(
        halves(before), halves(jnp.concatenate([head, nothing], axis=0)), LAST
    )

    def pack_copy(step):
        return pltpu.make_async_remote_copy(
            src_ref=pack.at[row], dst_ref=pack.at[row], send_sem=pack_send, recv_sem=pack_recv,
            device_id={"row": lax.rem(row + step, rows)}, device_id_type=pl.DeviceIdType.MESH,
        )

    def pack_others():
        ref = pack.at[pl.ds(0, rows - 1)]
        return pltpu.make_async_remote_copy(
            src_ref=ref, dst_ref=ref, send_sem=pack_send, recv_sem=pack_recv,
            device_id={"row": lax.rem(row + 1, rows)}, device_id_type=pl.DeviceIdType.MESH,
        )

    for step in range(1, rows):
        pack_copy(step).start()
    serve_all(0, 1)
    pack_others().wait_recv()

    square = pack[0, columns + 2 * own :, :]
    for index in range(1, rows):
        square = square + pack[index, columns + 2 * own :, :]
    square = square[:, :width_own]
    down = lax.broadcasted_iota(jnp.int32, (width_own, width_own), 0)
    over = lax.broadcasted_iota(jnp.int32, (width_own, width_own), 1)
    square = jnp.where(down < over, square, jnp.where(down == over, 0.5 * square, 0.0))
    square = triangle_inverse(square, down, over, width_own)
    square = jnp.concatenate([square, jnp.zeros((width_own, LANES - width_own), F32)], axis=1)
    folded = square[:8]
    for index in range(1, fold):
        folded = folded + pltpu.roll(square[8 * index : 8 * index + 8], index * width_own, 1)
    corner[side, at] = folded

    def send_corner(way, source):
        ref = corner.at[side, source]
        move = pltpu.make_async_remote_copy(
            src_ref=ref, dst_ref=ref, send_sem=corner_send.at[way],
            recv_sem=corner_across if way == ACROSS else corner_recv.at[source],
            device_id=target(way), device_id_type=pl.DeviceIdType.MESH,
        )
        guarded(way, move.start)

    def corner_wait(ref, way, sem):
        return pltpu.make_async_remote_copy(
            src_ref=ref, dst_ref=ref, send_sem=corner_send.at[way], recv_sem=sem,
            device_id=target(way), device_id_type=pl.DeviceIdType.MESH,
        )

    def serve_corner(step):
        for way, source in ((UP, at - step), (DOWN, at + step)):
            @pl.when((source >= 0) & (source < line))
            def _(way=way, source=source):
                corner_wait(corner.at[side, source], ACROSS, corner_recv.at[source]).wait_recv()
                send_corner(way, source)
                send_corner(ACROSS, source)

    for way in (UP, DOWN, ACROSS):
        send_corner(way, at)

    def placed(value, shift):
        wide = value
        if total > 2 * own:
            zeros = jnp.zeros((value.shape[0], total - 2 * own), F32)
            wide = jnp.concatenate([value, zeros], axis=1)
        shift = shift * own % total
        return pltpu.roll(wide, shift, 1) if shift else wide

    inner = jnp.zeros((columns, total), F32)
    bands = []
    for index in range(rows):
        inner = inner + placed(pack[index, :columns, :], index - 1)
        block = placed(pack[index, columns : columns + own, :], index - 1)
        if index < rows - 1:
            block = block + placed(pack[index + 1, columns + own : columns + 2 * own, :], index + 1)
        bands.append(block)
    matrix = jnp.concatenate(bands, axis=0)
    orders = []
    for axis in range(2):
        value = lax.broadcasted_iota(jnp.int32, (total, total), axis)
        part, within = value // own, value % own
        sweep_own = spans * refl
        orders.append((within // sweep_own) * (rows * sweep_own) + part * sweep_own + within % sweep_own)
    down, over = orders
    earlier = (down // refl > over // refl) | ((down // refl == over // refl) & (down < over))
    matrix = jnp.where(earlier, matrix, jnp.where(down == over, 0.5 * matrix, 0.0))
    coeffs = precise_dot(inner, triangle_inverse(matrix, down, over, total), LAST)
    coeffs = pltpu.roll(coeffs, lax.rem(total + own - own * row, total), 1)[:, : 2 * own]
    coeffs = halves(coeffs)
    for step in range(2, line - 1):
        serve_all(0, step)

    @pl.loop(0, groups)
    def _(index):
        spread = spans_group(index)
        right = jnp.concatenate([jnp.zeros_like(spread), spread], axis=0)
        eig[:, cut_group(index)] -= dot_split(coeffs, halves(right), INNER)

    eig[:, :LANES] -= dot_split(coeffs, halves(jnp.concatenate([before, nothing], axis=0)), INNER)
    serve_all(0, line - 1)
    serve_corner(1)
    for panel in range(1, panels):
        send_own(ACROSS, panel)

    def reflectors(panel, where, parts):
        return jnp.concatenate([walls[panel][part[0], part[1], :, where] for part in parts], axis=0)

    def rounded(where):
        return eig[:, where].astype(BF16)

    def row_copy(source, dest, send, recv, step):
        bit = 2**step
        low_bit = (row // bit) % 2
        return pltpu.make_async_remote_copy(
            src_ref=source, dst_ref=dest, send_sem=send, recv_sem=recv,
            device_id={"row": row + bit * (1 - 2 * low_bit)}, device_id_type=pl.DeviceIdType.MESH,
        )

    steps = rows.bit_length() - 1
    kept = (columns + width, columns + early_width)

    def row_sum(panel, meanwhile):
        rows_at = pl.ds(0, kept[panel])
        for step in range(steps):
            move = row_copy(
                sums.at[panel, rows_at], got.at[panel, step, rows_at],
                sum_send.at[panel, step], sum_recv.at[panel, step], step,
            )
            move.start()
            if step == steps - 1:
                meanwhile()
            move.wait()
            sums[panel, rows_at, :] += got[panel, step, rows_at, :]

    def triangle(gram):
        down = lax.broadcasted_iota(jnp.int32, (width, width), 0)
        over = lax.broadcasted_iota(jnp.int32, (width, width), 1)
        matrix = jnp.where(down < over, gram, jnp.where(down == over, 0.5 * gram, 0.0))
        return triangle_inverse(matrix, down, over, width)

    def diagonal(parts):
        stack = []
        for part in parts:
            folded = corner[part[0], part[1]]
            stack.append(folded)
            for index in range(1, fold):
                stack.append(pltpu.roll(folded, LANES - index * width_own, 1))
        stack = jnp.concatenate(stack, axis=0)
        down = lax.broadcasted_iota(jnp.int32, (LANES, width), 0)
        over = lax.broadcasted_iota(jnp.int32, (LANES, width), 1) % width_own
        wide = precise_dot(stack, jnp.where(down == over, 1.0, 0.0).astype(F32))
        down = lax.broadcasted_iota(jnp.int32, (width, width), 0) // width_own
        over = lax.broadcasted_iota(jnp.int32, (width, width), 1) // width_own
        return jnp.where(down == over, wide, 0.0)

    def set_places(parts):
        for axis in range(2):
            part_at = lax.broadcasted_iota(jnp.int32, (width, width), axis) // width_own
            place = jnp.zeros_like(part_at)
            for index, part in enumerate(parts):
                place = jnp.where(part_at == index, 2 * part[1] + part[0], place)
            places[axis] = place

    def solved(gram, inner, inverse):
        down, over = places[0], places[1]
        if cols > 8:
            size = 1
            while size < cols:
                off = (down // (2 * size) == over // (2 * size)) & (down // size < over // size)
                off = halves(jnp.where(off, gram, 0.0))
                split = halves(inverse)
                inverse = inverse - dot_split(split, halves(dot_split(off, split, INNER)), INNER)
                size *= 2
            return dot_split(halves(inner), halves(inverse), LAST).astype(BF16)
        split = halves(inverse)
        power = halves(dot_split(split, halves(jnp.where(down < over, gram, 0.0)), INNER))
        value = dot_split(halves(inner), split, LAST)
        value = value - dot_split(halves(value), power, LAST)
        size = 2
        while size < cols:
            power = halves(dot_split(power, power, INNER))
            value = value + dot_split(halves(value), power, LAST)
            size *= 2
        return value.astype(BF16)

    for panel in range(panels):
        sums[panel] = jnp.zeros_like(sums[panel])
    late[...] = jnp.zeros_like(late)
    bulk[...] = jnp.zeros_like(bulk)
    for part in range(2):
        arrived(0, walls[0].at[other, :, :, span_of(part)], first_sem.at[part])

        @pl.loop(bounds[part], bounds[part + 1])
        def _(index):
            reflect = reflectors(0, cut(index), natural)
            left = jnp.concatenate([rounded(cut(index)), reflect], axis=0)
            sums[0] += lax.dot_general(left, reflect, LAST, preferred_element_type=F32)

        serve(1, 1, part)

    def serve_between():
        for step in range(2, line - 1):
            for part in range(2):
                serve(1, step, part)
        for part in range(2):
            serve_partner(part)

    serve_corner(2)
    row_sum(0, serve_between)
    for step in range(3, line):
        serve_corner(step)
    coeffs = precise_dot(sums[0, :columns, :], triangle(sums[0, columns:, :]), LAST).astype(BF16)

    @pl.loop(0, chunks)
    def _(index):
        reflect = reflectors(0, cut(index), natural)
        eig[:, cut(index)] -= lax.dot_general(coeffs, reflect, INNER, preferred_element_type=F32)

    early_parts, late_parts = order[:-2], order[-2:]

    for part in range(2):
        serve(1, line - 1, part)
        arrived(1, walls[1].at[other, pl.ds(0, line - 3), :, span_of(part)], early_sem.at[part])

        @pl.loop(bounds[part], bounds[part + 1])
        def _(index):
            reflect = reflectors(1, cut(index), early_parts)
            left = jnp.concatenate([rounded(cut(index)), reflect], axis=0)
            right = jnp.concatenate([reflect, jnp.zeros((late_width, chunk), BF16)], axis=0)
            sums[1, pl.ds(0, kept[1]), :] += lax.dot_general(left, right, LAST, preferred_element_type=F32)

    def add_late(where, sem, into):
        arrived(1, walls[1].at[other, pl.ds(0, 2), :, where], sem)
        reflect = reflectors(1, where, late_parts)
        right = jnp.concatenate([reflectors(1, where, order), rounded(where)], axis=0)
        into[...] += lax.dot_general(reflect, right, LAST, preferred_element_type=F32)

    def prepare():
        corner_wait(corner.at[other], ACROSS, corner_across).wait_recv()
        set_places(order)
        blocks[...] = diagonal(order)
        pl.loop(0, max(chunks - 2, 0))(lambda index: add_late(cut(index), last_sem.at[index], bulk))

    row_sum(1, prepare)
    def bulk_move(step):
        return row_copy(bulk, bulk_got.at[step], bulk_send.at[step], bulk_recv.at[step], step)

    bulk_move(0).start()
    for index in range(max(chunks - 2, 0), chunks - 1):
        add_late(cut(index), last_sem.at[index], late)
    for step in range(1, steps):
        bulk_move(step - 1).wait()
        bulk[...] += bulk_got[step - 1]
        bulk_move(step).start()
    for index, where in enumerate(closing):
        add_late(where, last_sem.at[chunks - 1 + index], late)

    def gone(ref, way, sem):
        pltpu.make_async_remote_copy(
            src_ref=ref, dst_ref=ref, send_sem=sem, recv_sem=partner_sem.at[0], device_id=target(way),
            device_id_type=pl.DeviceIdType.MESH,
        ).wait_send()

    def all_gone():
        for panel in range(panels):
            pieces = walls[panel].at[0]
            for place in range(line):
                @pl.when(at == place)
                def _(place=place):
                    above, below = place + 1, line - place
                    if panel == last:
                        above, below = above + 1 - place % 2, below + place % 2
                    if place < line - 1:
                        gone(pieces.at[pl.ds(0, above)], UP, send_sem.at[UP, panel])
                    if place > 0:
                        gone(pieces.at[pl.ds(0, below)], DOWN, send_sem.at[DOWN, panel])
            count = line - 1 if panel == last else line
            gone(pieces.at[pl.ds(0, count)], ACROSS, send_sem.at[ACROSS, panel])
        for place in range(line):
            @pl.when(at == place)
            def _(place=place):
                if place < line - 1:
                    corner_wait(corner.at[0, pl.ds(0, place + 1)], UP, corner_across).wait_send()
                if place > 0:
                    corner_wait(corner.at[0, pl.ds(0, line - place)], DOWN, corner_across).wait_send()
        corner_wait(corner.at[0], ACROSS, corner_across).wait_send()
        pl.when(row < rows - 1)(lambda: tail_copy().wait_send())
        pack_others().wait_send()

    for step in range(steps):
        if step == 0:
            move = row_copy(late, late_got, late_send.at[step], late_recv.at[step], step)
        else:
            late_cast[...] = late[...].astype(BF16)
            move = row_copy(late_cast, late_cast_got.at[step - 1], late_send.at[step], late_recv.at[step], step)
        move.start()
        if step == steps - 1:
            all_gone()
            bulk_move(step).wait()
            bulk[...] += bulk_got[step]
        move.wait()
        late[...] += late_got[...] if step == 0 else late_cast_got[step - 1].astype(F32)
    summed = late[...] + bulk[...]
    down = lax.broadcasted_iota(jnp.int32, (late_width, width), 0)
    over = lax.broadcasted_iota(jnp.int32, (late_width, width), 1)
    turn = jnp.where(down + early_width == over, 1.0, 0.0).astype(BF16)
    first_dim = (((0,), (0,)), ((), ()))
    turned = sum(lax.dot_general(part, turn, first_dim, preferred_element_type=F32) for part in halves(summed))
    gram = jnp.concatenate(
        [sums[1, columns : columns + early_width, :] + turned[:early_width], summed[:, :width]], axis=0
    )
    coef_ref[...] = solved(gram, sums[1, :columns, :] + turned[width:], blocks[...])


def finish_kernel(eig_ref, wall_ref, coef_ref, out_ref, held, sems):
    line = wall_ref.shape[1]
    rows_dev = eig_ref.shape[1]
    chunk = tile_of(rows_dev, 14)
    chunks = rows_dev // chunk

    def cut(index):
        return pl.ds(pl.multiple_of(index * chunk, chunk), chunk)

    def copy(index):
        return pltpu.make_async_copy(held.at[:, cut(index)], out_ref.at[:, cut(index)], sems.at[index])

    coeffs = coef_ref[...]
    col = lax.axis_index("col")
    order = last_order(line, col // 2, col % 2)

    for index in range(chunks):
        reflect = jnp.concatenate([wall_ref[part[0], part[1], :, cut(index)] for part in order], axis=0)
        update = lax.dot_general(coeffs, reflect, INNER, preferred_element_type=F32)
        held[:, cut(index)] = eig_ref[:, cut(index)] - update
        copy(index).start()

    @pl.loop(0, chunks)
    def _(index):
        copy(index).wait()


def local(eigvecs, span_vectors, span_offsets, panels):
    rows, cols = lax.axis_size("row"), lax.axis_size("col")
    columns, rows_dev = eigvecs.shape
    count, width_own, _ = panels.shape
    sweeps, spans, refl, band = span_vectors.shape
    own = sweeps * spans * refl
    width = width_own * cols
    steps = rows.bit_length() - 1
    chunks = rows_dev // tile_of(rows_dev, 14)
    late_width = 2 * width_own
    line = cols // 2
    vmem = pltpu.VMEM
    dma = pltpu.SemaphoreType.DMA
    eigen, wall, coeffs = pl.pallas_call(
        kernel,
        out_shape=(
            vmem(eigvecs.shape, F32),
            vmem((2, line, width_own, rows_dev), BF16),
            vmem((columns, width), BF16),
        ),
        in_specs=[pl.BlockSpec(memory_space=pltpu.HBM)] * 4,
        out_specs=[pl.BlockSpec(memory_space=pltpu.VMEM)] * 3,
        scratch_shapes=[
            vmem((2, line, width_own, rows_dev), BF16),
            vmem(span_vectors.shape, F32),
            pltpu.SMEM(span_offsets.shape, jnp.int32),
            vmem((own, LANES), F32),
            vmem((own, LANES), F32),
            vmem((own, LANES), jnp.int32),
            vmem((own, LANES), F32),
            vmem((own, LANES), F32),
            vmem((rows, columns + 2 * own + width_own, 2 * own), F32),
            vmem((count, columns + width, width), F32),
            vmem((count, steps, columns + width, width), F32),
            vmem((late_width, columns + width), F32),
            vmem((late_width, columns + width), F32),
            vmem((late_width, columns + width), BF16),
            vmem((steps, late_width, columns + width), BF16),
            vmem((late_width, columns + width), F32),
            vmem((steps, late_width, columns + width), F32),
            vmem((2, line, 8, LANES), F32),
            vmem((2, width, width), jnp.int32),
            vmem((width, width), F32),
            dma((3,)),
            dma((count,)),
            dma((count, line, 2)),
            dma((2,)),
            dma((2,)),
            dma((2,)),
            dma((chunks + 1,)),
            dma((3, count)),
            dma((2,)),
            dma,
            dma,
            dma((count, steps)),
            dma((count, steps)),
            dma((steps,)),
            dma((steps,)),
            dma((steps,)),
            dma((steps,)),
            dma((3,)),
            dma((line,)),
            dma,
        ],
        compiler_params=pltpu.CompilerParams(
            collective_id=0, has_side_effects=True, vmem_limit_bytes=40 * 2**20
        ),
        cost_estimate=pl.CostEstimate(
            flops=8 * width * (width + columns) * rows_dev,
            bytes_accessed=8 * rows_dev * columns + 8 * width * rows_dev,
            transcendentals=0,
        ),
    )(*(pltpu.with_memory_space_constraint(value, pltpu.HBM) for value in (eigvecs, span_vectors, span_offsets, panels)))
    return pl.pallas_call(
        finish_kernel,
        out_shape=jax.ShapeDtypeStruct(eigvecs.shape, F32),
        in_specs=[pl.BlockSpec(memory_space=pltpu.VMEM)] * 3,
        out_specs=pl.BlockSpec(memory_space=pl.ANY),
        scratch_shapes=[vmem(eigvecs.shape, F32), dma((rows_dev // tile_of(rows_dev, 14),))],
        compiler_params=pltpu.CompilerParams(vmem_limit_bytes=16 * 2**20),
        cost_estimate=pl.CostEstimate(
            flops=2 * width * columns * rows_dev, bytes_accessed=8 * columns * rows_dev, transcendentals=0
        ),
    )(eigen, wall, coeffs)


def solution(mesh):
    return jax.shard_map(
        local,
        mesh=mesh,
        in_specs=(
            P("col", "row"),
            P(None, "row", None, None),
            P(None, "row"),
            P(None, "col", "row"),
        ),
        out_specs=P("col", "row"),
        check_vma=False,
    )
```
